8 devices in a mesh: dp: 2 (over z, y), sp: 4 (over x, core).
Axes of the slice: x: 2, y: 2, z: 1, core: 2. Of those that a mesh axis runs over, the one named last changes fastest.
Arguments:
- hidden: bfloat16 [4096, 5120], P(('dp', 'sp')), parts along dimension 0
- ln_gain: bfloat16 [5120], replicated
- w_q: bfloat16 [5120, 8192], replicated
- w_k: bfloat16 [5120, 1024], replicated
- w_v: bfloat16 [5120, 1024], replicated
- w_o: bfloat16 [8192, 5120], replicated
- q_gain: bfloat16 [128], replicated
- k_gain: bfloat16 [128], replicated
Outputs:
- output: bfloat16 [4096, 5120], P(('dp', 'sp')), parts along dimension 0
There are 2 independent parts. The reference program is written for one: setup_inputs(seed, part) draws one part's arguments, and reference() takes and returns one part's arrays. A program takes and returns all parts, laid end to end along the dimension named above; an argument that names none is the same for every part.
All inputs are finite; a program needn't handle non-finite values.
Results may differ from the reference program's by a relative error of at most 0.00696765.
Values are sent between devices in bfloat16 or wider.
A program may use at most 1 GiB of HBM per device.

```python
import math
import jax
import jax.numpy as jnp
from jax import lax

D = 5120
HEADS = 64
KV_HEADS = 8
HEAD = 128
SEQ = 2048
EPS = 1e-6
THETA = 1000000.0


def setup_inputs(seed: int = 0, part: int = 0) -> dict:
    keys = jax.random.split(jax.random.key(seed), 7)
    part_key = jax.random.fold_in(jax.random.key(seed + 1), part)
    gain_scale = math.log(SEQ / 8.0) ** 0.25
    hidden = jax.random.normal(part_key, (SEQ, D), jnp.float32)
    ln_gain = 1.0 + 0.3 * jax.random.normal(keys[0], (D,), jnp.float32)
    w_q = jax.random.normal(keys[1], (D, HEADS * HEAD), jnp.float32) * D ** -0.5
    w_k = jax.random.normal(keys[2], (D, KV_HEADS * HEAD), jnp.float32) * D ** -0.5
    w_v = jax.random.normal(keys[3], (D, KV_HEADS * HEAD), jnp.float32) * D ** -0.5
    w_o = jax.random.normal(keys[4], (HEADS * HEAD, D), jnp.float32) * (2.0 * (HEADS * HEAD) ** -0.5)
    q_gain = gain_scale * (1.0 + 0.2 * jax.random.normal(keys[5], (HEAD,), jnp.float32))
    k_gain = gain_scale * (1.0 + 0.2 * jax.random.normal(keys[6], (HEAD,), jnp.float32))
    return {
        'hidden': hidden.astype(jnp.bfloat16),
        'ln_gain': ln_gain.astype(jnp.bfloat16),
        'w_q': w_q.astype(jnp.bfloat16),
        'w_k': w_k.astype(jnp.bfloat16),
        'w_v': w_v.astype(jnp.bfloat16),
        'w_o': w_o.astype(jnp.bfloat16),
        'q_gain': q_gain.astype(jnp.bfloat16),
        'k_gain': k_gain.astype(jnp.bfloat16),
    }


def head_norm(values, gain):
    return values * lax.rsqrt(jnp.mean(values * values, axis=-1, keepdims=True) + EPS) * gain.astype(jnp.float32)


def rotate(values, positions):
    half = HEAD // 2
    inv_freq = jnp.power(THETA, -(jnp.arange(half, dtype=jnp.float32) * (2.0 / HEAD)))
    angles = positions.astype(jnp.float32)[:, None] * inv_freq[None, :]
    cos_pos = jnp.cos(angles)[:, None, :]
    sin_pos = jnp.sin(angles)[:, None, :]
    first_half = values[..., :half]
    second_half = values[..., half:]
    return jnp.concatenate([first_half * cos_pos - second_half * sin_pos, second_half * cos_pos + first_half * sin_pos], axis=-1)


def attend(q_all, k_all, v_all):
    limit = 2 ** 25 // (HEADS * SEQ)
    block_rows = min(SEQ, 2 ** max(3, min(9, limit.bit_length() - 1)))
    num_blocks = SEQ // block_rows
    group = HEADS // KV_HEADS
    q_blocks = q_all.reshape(num_blocks, block_rows, KV_HEADS, group, HEAD)
    key_pos = jnp.arange(SEQ)
    k_f32 = k_all.astype(jnp.float32)
    v_f32 = v_all.astype(jnp.float32)

    def one_block(block_args):
        q_block, block_idx = block_args
        scores = jnp.einsum('qkgd,skd->kgqs', q_block.astype(jnp.float32), k_f32) * (HEAD ** -0.5)
        q_pos = block_idx * block_rows + jnp.arange(block_rows)
        visible = q_pos[:, None] >= key_pos[None, :]
        scores = jnp.where(visible, scores, -jnp.inf)
        attn_prob = jax.nn.softmax(scores, axis=-1).astype(jnp.bfloat16)
        mixed = jnp.einsum('kgqs,skd->qkgd', attn_prob.astype(jnp.float32), v_f32)
        return mixed.astype(jnp.bfloat16)

    outputs = lax.map(one_block, (q_blocks, jnp.arange(num_blocks)))
    return outputs.reshape(SEQ, HEADS, HEAD)


def reference(hidden, ln_gain, w_q, w_k, w_v, w_o, q_gain, k_gain):
    hidden_f32 = hidden.astype(jnp.float32)
    normed = (hidden_f32 * lax.rsqrt(jnp.mean(hidden_f32 * hidden_f32, axis=-1, keepdims=True) + EPS) * ln_gain.astype(jnp.float32)).astype(jnp.bfloat16)
    positions = jnp.arange(SEQ)
    q_raw = jnp.dot(normed, w_q, preferred_element_type=jnp.float32).reshape(SEQ, HEADS, HEAD)
    k_raw = jnp.dot(normed, w_k, preferred_element_type=jnp.float32).reshape(SEQ, KV_HEADS, HEAD)
    v_all = jnp.dot(normed, w_v, preferred_element_type=jnp.float32).astype(jnp.bfloat16).reshape(SEQ, KV_HEADS, HEAD)
    q_all = rotate(head_norm(q_raw, q_gain), positions).astype(jnp.bfloat16)
    k_all = rotate(head_norm(k_raw, k_gain), positions).astype(jnp.bfloat16)
    mixed = attend(q_all, k_all, v_all)
    result = hidden_f32 + jnp.dot(mixed.reshape(SEQ, HEADS * HEAD), w_o, preferred_element_type=jnp.float32)
    return result.astype(jnp.bfloat16)
```

```python
import functools
import math

import jax
import jax.numpy as jnp
from jax import lax
from jax.experimental import pallas as pl
from jax.experimental.pallas import tpu as pltpu
from jax.sharding import PartitionSpec as P

EPS = 1e-6
THETA = 1000000.0
HD = 128
VMEM_LIMIT = 60 * 1024 * 1024
NT = (((1,), (1,)), ((), ()))
F32 = jnp.float32
BF16 = jnp.bfloat16
ANY = pl.BlockSpec(memory_space=pl.ANY)


def rope_tables(positions, gain):
    half = HD // 2
    inv_freq = jnp.power(THETA, -(jnp.arange(half, dtype=F32) * (2.0 / HD)))
    angles = positions.astype(F32)[:, None] * inv_freq[None, :]
    cos = jnp.cos(angles)
    sin = jnp.sin(angles)
    gain = gain.astype(F32)
    swapped = jnp.concatenate([gain[half:], gain[:half]])
    cos_g = jnp.concatenate([cos, cos], axis=1) * gain[None, :]
    sin_g = jnp.concatenate([-sin, sin], axis=1) * swapped[None, :]
    return cos_g, sin_g


def norm_rope(acc, cos_g, sin_g):
    var = jnp.mean(acc * acc, axis=-1, keepdims=True)
    n = acc * lax.rsqrt(var + EPS)
    return (n * cos_g + pltpu.roll(n, HD // 2, 1) * sin_g).astype(BF16)


def kv_kernel(meta, h_ref, wk_ref, wv_ref, cos_ref, sin_ref, own_ref, other_ref):
    n = pl.program_id(0)
    k = jnp.dot(h_ref[...], wk_ref[...], preferred_element_type=F32)
    v = jnp.dot(h_ref[...], wv_ref[...], preferred_element_type=F32)
    cos_g = cos_ref[...]
    sin_g = sin_ref[...]

    def put(out_ref, base):
        for i in range(2):
            cols = slice(i * HD, (i + 1) * HD)
            out_ref[0, base + i] = norm_rope(k[:, cols], cos_g, sin_g)
            out_ref[1, base + i] = v[:, cols].astype(BF16)

    for step in range(4):
        @pl.when(n == step)
        def _():
            put(own_ref if step < 2 else other_ref, (step % 2) * 2)


def kv_project(core, h, w_k, w_v, cos_g, sin_g):
    rows, dim = h.shape
    meta = jnp.stack([core]).astype(jnp.int32)
    wspec = pl.BlockSpec((dim, 256), lambda n, m: (0, (n + 2 * m[0]) % 4))
    full = lambda *s: pl.BlockSpec(s, lambda n, m: (0,) * len(s), pipeline_mode=pl.Buffered(1))
    out = jax.ShapeDtypeStruct((2, 4, rows, HD), BF16)
    return pl.pallas_call(
        kv_kernel,
        grid_spec=pltpu.PrefetchScalarGridSpec(
            num_scalar_prefetch=1,
            grid=(4,),
            in_specs=[full(rows, dim), wspec, wspec, full(rows, HD), full(rows, HD)],
            out_specs=[full(2, 4, rows, HD), full(2, 4, rows, HD)],
        ),
        out_shape=[out, out],
        compiler_params=pltpu.CompilerParams(vmem_limit_bytes=VMEM_LIMIT),
        cost_estimate=pl.CostEstimate(flops=4 * rows * dim * 1024, bytes_accessed=4 * dim * 1024, transcendentals=0),
        name='kv_proj',
    )(meta, h, w_k, w_v, cos_g, sin_g)


def q_kernel(meta, own_hbm, part_hbm, w_ref, cos_ref, sin_ref, q_ref, h_scr, sems):
    n = pl.program_id(0)
    core = meta[0]
    rows = own_hbm.shape[0]
    mine = pltpu.make_async_copy(own_hbm, h_scr.at[pl.ds(pl.multiple_of(core * rows, rows), rows)], sems.at[0])
    theirs = pltpu.make_async_copy(part_hbm, h_scr.at[pl.ds(pl.multiple_of((1 - core) * rows, rows), rows)], sems.at[1])

    @pl.when(n == 0)
    def _():
        mine.start()
        theirs.start()
        mine.wait()
        theirs.wait()

    heads = w_ref.shape[1] // HD
    for lo in range(0, 2 * rows, 512):
        r = slice(lo, lo + 512)
        acc = jnp.dot(h_scr[r, :], w_ref[...], preferred_element_type=F32)
        for i in range(heads):
            q_ref[i, r, :] = norm_rope(acc[:, i * HD:(i + 1) * HD], cos_ref[r, :], sin_ref[r, :])


def q_project(core, h_own, h_part, w_q, cos_g, sin_g):
    rows, dim = h_own.shape
    bn = 256
    steps = w_q.shape[1] // 2 // bn
    meta = jnp.stack([core]).astype(jnp.int32)
    full = lambda *s: pl.BlockSpec(s, lambda n, m: (0,) * len(s), pipeline_mode=pl.Buffered(1))
    return pl.pallas_call(
        q_kernel,
        grid_spec=pltpu.PrefetchScalarGridSpec(
            num_scalar_prefetch=1,
            grid=(steps,),
            in_specs=[ANY, ANY, pl.BlockSpec((dim, bn), lambda n, m: (0, n + steps * m[0])), full(2 * rows, HD), full(2 * rows, HD)],
            out_specs=pl.BlockSpec((bn // HD, 2 * rows, HD), lambda n, m: (n, 0, 0)),
            scratch_shapes=[pltpu.VMEM((2 * rows, dim), BF16), pltpu.SemaphoreType.DMA((2,))],
        ),
        out_shape=jax.ShapeDtypeStruct((steps * bn // HD, 2 * rows, HD), BF16),
        compiler_params=pltpu.CompilerParams(vmem_limit_bytes=VMEM_LIMIT),
        cost_estimate=pl.CostEstimate(flops=4 * rows * dim * bn * steps, bytes_accessed=2 * dim * bn * steps, transcendentals=0),
        name='q_proj',
    )(meta, h_own, h_part, w_q, cos_g, sin_g)


TILE = 128
KB = 512


def attn_kernel(meta, q_ref, own_hbm, part_hbm, same_hbm, cross_hbm, keep_ref, send_ref, k_scr, v_scr, s_scr, m_scr, acc_scr, sems):
    g = pl.program_id(0)
    t = pl.program_id(1)
    chip = meta[0]
    core = meta[1]
    rows = own_hbm.shape[2]
    group = q_ref.shape[0]
    scale = HD ** -0.5 * math.log2(math.e)

    def pieces(c, x):
        own_at = x * 2 * rows + c * rows
        part_at = x * 2 * rows + (1 - c) * rows
        copies = []
        for i, scr in enumerate((k_scr, v_scr)):
            copies.append((own_hbm, i, scr, own_at))
            copies.append((part_hbm, i, scr, part_at))
            if x == 1:
                copies.append((same_hbm, i, scr, c * rows))
                copies.append((cross_hbm, i, scr, (1 - c) * rows))
        return [pltpu.make_async_copy(src.at[i], dst.at[:, pl.ds(at, rows)], sems.at[j]) for j, (src, i, dst, at) in enumerate(copies)]

    @pl.when(jnp.logical_and(g == 0, t == 0))
    def _():
        for x in range(2):
            for c in range(2):
                @pl.when(jnp.logical_and(chip == x, core == c))
                def _():
                    cps = pieces(c, x)
                    for cp in cps:
                        cp.start()
                    for cp in cps:
                        cp.wait()

    pos0 = chip * 2 * rows + t * TILE
    nfull = pos0 // KB
    m_rows = group * TILE
    q = q_ref[...].reshape(m_rows, HD)

    def score(j):
        kb = k_scr[g, pl.ds(pl.multiple_of(j * KB, KB), KB), :]
        return lax.dot_general(q, kb, NT, preferred_element_type=F32)

    def lane_max(s):
        m = s[:, :HD]
        for i in range(1, KB // HD):
            m = jnp.maximum(m, s[:, i * HD:(i + 1) * HD])
        return m

    s = score(nfull)
    off = pos0 - nfull * KB
    row = lax.broadcasted_iota(jnp.int32, (group, TILE, KB), 1).reshape(m_rows, KB) + off
    col = lax.broadcasted_iota(jnp.int32, (m_rows, KB), 1)
    s = jnp.where(row >= col, s, -jnp.inf)
    s_scr[nfull] = s
    m_scr[...] = lane_max(s)

    def first(j, _):
        s = score(j)
        s_scr[j] = s
        m_scr[...] = jnp.maximum(m_scr[...], lane_max(s))
        return 0

    lax.fori_loop(0, nfull, first, 0)
    m = jnp.max(m_scr[...], axis=1, keepdims=True) * scale
    m_scr[...] = jnp.broadcast_to(m, m_scr.shape)
    acc_scr[...] = jnp.zeros_like(acc_scr)

    def second(j, _):
        m = m_scr[:, :1]
        p = jnp.exp2(s_scr[j] * scale - m).astype(BF16)
        vb = v_scr[g, pl.ds(pl.multiple_of(j * KB, KB), KB), :]
        ve = jnp.concatenate([vb, jnp.ones((KB, HD), BF16)], axis=1)
        acc_scr[...] += jnp.dot(p, ve, preferred_element_type=F32)
        return 0

    lax.fori_loop(0, nfull + 1, second, 0)
    acc = acc_scr[...]
    o = (acc[:, :HD] / acc[:, HD:]).astype(BF16).reshape(group, TILE, HD)
    per = rows // TILE
    at = pl.ds(pl.multiple_of((t % per) * TILE, TILE), TILE)

    @pl.when(t // per == core)
    def _():
        for i in range(group):
            keep_ref[at, i * HD:(i + 1) * HD] = o[i]

    @pl.when(t // per != core)
    def _():
        for i in range(group):
            send_ref[at, i * HD:(i + 1) * HD] = o[i]


def attention(chip, core, q, kv_own, kv_part, kv_same, kv_cross):
    heads, q_rows, _ = q.shape
    rows = q_rows // 2
    seq = 4 * rows
    group = 8
    meta = jnp.stack([chip, core]).astype(jnp.int32)
    out = jax.ShapeDtypeStruct((rows, heads * HD), BF16)
    ospec = pl.BlockSpec((rows, group * HD), lambda g, t, m: (0, g))
    return pl.pallas_call(
        attn_kernel,
        grid_spec=pltpu.PrefetchScalarGridSpec(
            num_scalar_prefetch=1,
            grid=(heads // group, q_rows // TILE),
            in_specs=[pl.BlockSpec((group, TILE, HD), lambda g, t, m: (g, t, 0)), ANY, ANY, ANY, ANY],
            out_specs=[ospec, ospec],
            scratch_shapes=[
                pltpu.VMEM((heads // group, seq, HD), BF16),
                pltpu.VMEM((heads // group, seq, HD), BF16),
                pltpu.VMEM((seq // KB, group * TILE, KB), F32),
                pltpu.VMEM((group * TILE, HD), F32),
                pltpu.VMEM((group * TILE, 2 * HD), F32),
                pltpu.SemaphoreType.DMA((8,)),
            ],
        ),
        out_shape=[out, out],
        compiler_params=pltpu.CompilerParams(vmem_limit_bytes=VMEM_LIMIT),
        cost_estimate=pl.CostEstimate(flops=4 * heads * q_rows * seq * HD, bytes_accessed=6 * heads * q_rows * HD, transcendentals=0),
        name='attn',
    )(meta, q, kv_own, kv_part, kv_same, kv_cross)


def out_kernel(meta, keep_ref, recv_ref, wa_ref, wb_ref, x_ref, o_ref):
    acc = jnp.dot(keep_ref[...], wa_ref[...], preferred_element_type=F32)
    acc += jnp.dot(recv_ref[...], wb_ref[...], preferred_element_type=F32)
    o_ref[...] = (acc + x_ref[...].astype(F32)).astype(BF16)


def out_project(core, keep, recv, w_o, x):
    rows, half = keep.shape
    dim = w_o.shape[1]
    bn = 256
    meta = jnp.stack([core]).astype(jnp.int32)
    full = pl.BlockSpec((rows, half), lambda n, m: (0, 0), pipeline_mode=pl.Buffered(1))
    tile = pl.BlockSpec((rows, bn), lambda n, m: (0, n))
    return pl.pallas_call(
        out_kernel,
        grid_spec=pltpu.PrefetchScalarGridSpec(
            num_scalar_prefetch=1,
            grid=(dim // bn,),
            in_specs=[full, full, pl.BlockSpec((half, bn), lambda n, m: (m[0], n)), pl.BlockSpec((half, bn), lambda n, m: (1 - m[0], n)), tile],
            out_specs=tile,
        ),
        out_shape=jax.ShapeDtypeStruct((rows, dim), BF16),
        compiler_params=pltpu.CompilerParams(vmem_limit_bytes=VMEM_LIMIT),
        cost_estimate=pl.CostEstimate(flops=4 * rows * half * dim, bytes_accessed=4 * half * dim, transcendentals=0),
        name='out_proj',
    )(meta, keep, recv, w_o, w_o, x)


PARTNER = [(0, 1), (1, 0), (2, 3), (3, 2)]


def solution(mesh):
    def device_step(hidden, ln_gain, w_q, w_k, w_v, w_o, q_gain, k_gain):
        rows = hidden.shape[0]
        sp = lax.axis_index('sp')
        chip = sp // 2
        core = sp % 2
        x = hidden.astype(F32)
        h = (x * lax.rsqrt(jnp.mean(x * x, axis=-1, keepdims=True) + EPS) * ln_gain.astype(F32)).astype(BF16)
        h_part = lax.ppermute(h, 'sp', PARTNER)
        cos_k, sin_k = rope_tables(sp * rows + jnp.arange(rows), k_gain)
        cos_q, sin_q = rope_tables(chip * 2 * rows + jnp.arange(2 * rows), q_gain)
        kv_own, kv_other = kv_project(core, h, w_k, w_v, cos_k, sin_k)
        kv_part = lax.ppermute(kv_other, 'sp', PARTNER)
        kv_same = lax.ppermute(kv_own, 'sp', [(0, 2), (1, 3)])
        kv_cross = lax.ppermute(kv_other, 'sp', [(0, 3), (1, 2)])
        q = q_project(core, h, h_part, w_q, cos_q, sin_q)
        keep, send = attention(chip, core, q, kv_own, kv_part, kv_same, kv_cross)
        recv = lax.ppermute(send, 'sp', PARTNER)
        return out_project(core, keep, recv, w_o, hidden)

    row_spec = P(('dp', 'sp'), None)
    return jax.shard_map(device_step, mesh=mesh, in_specs=(row_spec, P(), P(), P(), P(), P(), P(), P()), out_specs=row_spec, check_vma=False)
```

```python
import functools
import math

import jax
import jax.numpy as jnp
from jax import lax
from jax.experimental import pallas as pl
from jax.experimental.pallas import tpu as pltpu
from jax.sharding import PartitionSpec as P

EPS = 1e-6
THETA = 1000000.0
HD = 128
VMEM_LIMIT = 60 * 1024 * 1024
NT = (((1,), (1,)), ((), ()))
F32 = jnp.float32
BF16 = jnp.bfloat16
ANY = pl.BlockSpec(memory_space=pl.ANY)


def rope_tables(positions, gain):
    half = HD // 2
    inv_freq = jnp.power(THETA, -(jnp.arange(half, dtype=F32) * (2.0 / HD)))
    angles = positions.astype(F32)[:, None] * inv_freq[None, :]
    cos = jnp.cos(angles)
    sin = jnp.sin(angles)
    gain = gain.astype(F32)
    swapped = jnp.concatenate([gain[half:], gain[:half]])
    cos_g = jnp.concatenate([cos, cos], axis=1) * gain[None, :]
    sin_g = jnp.concatenate([-sin, sin], axis=1) * swapped[None, :]
    return cos_g, sin_g


def norm_rope(acc, cos_g, sin_g):
    var = jnp.mean(acc * acc, axis=-1, keepdims=True)
    n = acc * lax.rsqrt(var + EPS)
    return (n * cos_g + pltpu.roll(n, HD // 2, 1) * sin_g).astype(BF16)


def norm_kernel(x_ref, g_ref, h_ref):
    x = x_ref[...].astype(F32)
    n = x * lax.rsqrt(jnp.mean(x * x, axis=-1, keepdims=True) + EPS)
    h_ref[...] = (n * g_ref[...].astype(F32)).astype(BF16)


def rms_norm(x, gain):
    rows, dim = x.shape
    tile = pl.BlockSpec((64, dim), lambda i: (i, 0))
    return pl.pallas_call(
        norm_kernel,
        grid=(rows // 64,),
        in_specs=[tile, pl.BlockSpec((1, dim), lambda i: (0, 0))],
        out_specs=tile,
        out_shape=jax.ShapeDtypeStruct((rows, dim), BF16),
        cost_estimate=pl.CostEstimate(flops=4 * rows * dim, bytes_accessed=4 * rows * dim, transcendentals=0),
        name='norm',
    )(x, gain.reshape(1, dim))


def kv_kernel(meta, h_ref, wk_ref, wv_ref, cos_ref, sin_ref, own_ref, other_ref, k_scr, v_scr):
    n = pl.program_id(0)
    rows = h_ref.shape[0]

    def multiply(r):
        k_scr[r, :] = jnp.dot(h_ref[r, :], wk_ref[...], preferred_element_type=F32)
        v_scr[r, :] = jnp.dot(h_ref[r, :], wv_ref[...], preferred_element_type=F32)

    def put(step, r):
        out_ref = own_ref if step < 2 else other_ref
        for i in range(2):
            cols = slice(i * HD, (i + 1) * HD)
            out_ref[0, (step % 2) * 2 + i, r, :] = norm_rope(k_scr[r, cols], cos_ref[r, :], sin_ref[r, :])
            out_ref[1, (step % 2) * 2 + i, r, :] = v_scr[r, cols].astype(BF16)

    for step in range(5):
        @pl.when(n == step)
        def _():
            for lo in range(0, rows, 256):
                r = slice(lo, lo + 256)
                if step > 0:
                    put(step - 1, r)
                if step < 4:
                    multiply(r)


def kv_project(core, h, w_k, w_v, cos_g, sin_g):
    rows, dim = h.shape
    meta = jnp.stack([core]).astype(jnp.int32)
    wspec = pl.BlockSpec((dim, 256), lambda n, m: (0, (jnp.minimum(n, 3) + 2 * m[0]) % 4))
    full = lambda *s: pl.BlockSpec(s, lambda n, m: (0,) * len(s), pipeline_mode=pl.Buffered(1))
    out = jax.ShapeDtypeStruct((2, 4, rows, HD), BF16)
    return pl.pallas_call(
        kv_kernel,
        grid_spec=pltpu.PrefetchScalarGridSpec(
            num_scalar_prefetch=1,
            grid=(5,),
            in_specs=[full(rows, dim), wspec, wspec, full(rows, HD), full(rows, HD)],
            out_specs=[full(2, 4, rows, HD), full(2, 4, rows, HD)],
            scratch_shapes=[pltpu.VMEM((rows, 256), F32), pltpu.VMEM((rows, 256), F32)],
        ),
        out_shape=[out, out],
        compiler_params=pltpu.CompilerParams(vmem_limit_bytes=VMEM_LIMIT),
        cost_estimate=pl.CostEstimate(flops=4 * rows * dim * 1024, bytes_accessed=4 * dim * 1024, transcendentals=0),
        name='kv_proj',
    )(meta, h, w_k, w_v, cos_g, sin_g)


def q_kernel(meta, own_hbm, part_hbm, w_ref, cos_ref, sin_ref, q_ref, h_scr, acc_scr, sems):
    n = pl.program_id(0)
    last = pl.num_programs(0) - 1
    core = meta[0]
    rows = own_hbm.shape[0]
    heads = w_ref.shape[1] // HD
    chunk = 256
    chunks = [slice(lo, lo + chunk) for lo in range(0, 2 * rows, chunk)]

    def load(i, src):
        lo = i * chunk
        return pltpu.make_async_copy(src.at[pl.ds(lo % rows, chunk)], h_scr.at[pl.ds(lo, chunk)], sems.at[i])

    def multiply(r):
        acc_scr[r, :] = jnp.dot(h_scr[r, :], w_ref[...], preferred_element_type=F32)

    def put(r):
        for i in range(heads):
            acc = acc_scr[r, i * HD:(i + 1) * HD]
            var = jnp.mean(acc * acc, axis=-1, keepdims=True)
            t = acc * lax.rsqrt(var + EPS)
            t = t * cos_ref[r, :] + pltpu.roll(t, HD // 2, 1) * sin_ref[r, :]
            length = jnp.sqrt(jnp.sum(t * t, axis=-1, keepdims=True))
            lane = lax.broadcasted_iota(jnp.int32, t.shape, 1)
            q_ref[i, r, :HD] = t.astype(BF16)
            q_ref[i, r, HD:] = jnp.where(lane == 0, length, 0.0).astype(BF16)

    @pl.when(n == 0)
    def _():
        for c in range(2):
            @pl.when(core == c)
            def _():
                for i in range(len(chunks)):
                    load(i, own_hbm if (i * chunk) // rows == c else part_hbm).start()
        for i, r in enumerate(chunks):
            load(i, own_hbm).wait()
            multiply(r)

    @pl.when(jnp.logical_and(n > 0, n < last))
    def _():
        for lo in range(0, 2 * rows, 512):
            put(slice(lo, lo + 512))
            multiply(slice(lo, lo + 512))

    @pl.when(n == last)
    def _():
        for r in chunks:
            put(r)


def q_project(core, h_own, h_part, w_q, cos_g, sin_g):
    rows, dim = h_own.shape
    bn = 256
    steps = w_q.shape[1] // 2 // bn
    meta = jnp.stack([core]).astype(jnp.int32)
    full = lambda *s: pl.BlockSpec(s, lambda n, m: (0,) * len(s), pipeline_mode=pl.Buffered(1))
    return pl.pallas_call(
        q_kernel,
        grid_spec=pltpu.PrefetchScalarGridSpec(
            num_scalar_prefetch=1,
            grid=(steps + 1,),
            in_specs=[ANY, ANY, pl.BlockSpec((dim, bn), lambda n, m: (0, jnp.minimum(n, steps - 1) + steps * m[0])), full(2 * rows, HD), full(2 * rows, HD)],
            out_specs=pl.BlockSpec((bn // HD, 2 * rows, 2 * HD), lambda n, m: (jnp.maximum(n - 1, 0), 0, 0)),
            scratch_shapes=[pltpu.VMEM((2 * rows, dim), BF16), pltpu.VMEM((2 * rows, bn), F32), pltpu.SemaphoreType.DMA((4,))],
        ),
        out_shape=jax.ShapeDtypeStruct((steps * bn // HD, 2 * rows, 2 * HD), BF16),
        compiler_params=pltpu.CompilerParams(vmem_limit_bytes=VMEM_LIMIT),
        cost_estimate=pl.CostEstimate(flops=4 * rows * dim * bn * steps, bytes_accessed=2 * dim * bn * steps, transcendentals=0),
        name='q_proj',
    )(meta, h_own, h_part, w_q, cos_g, sin_g)


TILE = 128
KB = 512
SMALL = 2.0 ** -90


def attn_kernel(meta, q_ref, q_hbm, own_hbm, part_hbm, same_hbm, cross_hbm, keep_ref, send_ref, k_scr, v_scr, o_scr, low_scr, qs_scr, s_scr, m_scr, sems, o_sems):
    g = pl.program_id(0)
    t = pl.program_id(1)
    tiles = pl.num_programs(1)
    chip = meta[0]
    core = meta[1]
    rows = own_hbm.shape[2]
    group = q_ref.shape[0]
    seq = k_scr.shape[1]
    scale = HD ** -0.5 * math.log2(math.e)
    per = rows // TILE

    def pieces(c, x):
        own_at = x * 2 * rows + c * rows
        part_at = x * 2 * rows + (1 - c) * rows
        copies = []
        for i, scr in enumerate((k_scr, v_scr)):
            copies.append((own_hbm, i, scr, own_at))
            copies.append((part_hbm, i, scr, part_at))
            if x == 1:
                copies.append((same_hbm, i, scr, c * rows))
                copies.append((cross_hbm, i, scr, (1 - c) * rows))
        return [
            pltpu.make_async_copy(src.at[i], dst.at[:, pl.ds(at, rows), pl.ds(0, HD)], sems.at[j])
            for j, (src, i, dst, at) in enumerate(copies)
        ]

    @pl.when(jnp.logical_and(g == 0, t == 0))
    def _():
        for x in range(2):
            for c in range(2):
                @pl.when(jnp.logical_and(chip == x, core == c))
                def _():
                    cps = pieces(c, x)
                    for cp in cps:
                        cp.start()
                    if x == 0:
                        k_scr[:, 2 * rows:, :HD] = jnp.zeros((k_scr.shape[0], 2 * rows, HD), BF16)
                    v_scr[:, :, HD:] = jnp.ones((v_scr.shape[0], seq, HD), BF16)
                    for cp in cps:
                        cp.wait()

    @pl.when(t == 0)
    def _():
        k = k_scr[g, :, :HD]
        sums = jnp.dot(k * k, jnp.ones((HD, HD), BF16), preferred_element_type=F32)
        longest = jnp.sqrt(jnp.max(sums)) * 1.02
        lane = lax.broadcasted_iota(jnp.int32, (seq, HD), 1)
        k_scr[g, :, HD:] = jnp.where(lane == 0, -longest, 0.0).astype(BF16)
        low_scr[...] = jnp.ones_like(low_scr)

    pos0 = chip * 2 * rows + t * TILE
    nfull = pos0 // KB
    off = pos0 - nfull * KB
    parts = 2
    hc = group // parts
    mc = hc * TILE

    it = g * tiles + t
    slot = it % 2

    def out_copy(ref, at_slot, at_tile, at_group):
        rows_at = pl.ds(pl.multiple_of((at_tile % per) * TILE, TILE), TILE)
        cols_at = pl.ds(pl.multiple_of(at_group * group * HD, group * HD), group * HD)
        return pltpu.make_async_copy(o_scr.at[at_slot], ref.at[rows_at, cols_at], o_sems.at[at_slot])

    def send_out(at_slot, at_tile):
        @pl.when(at_tile // per == core)
        def _():
            out_copy(keep_ref, at_slot, at_tile, g).start()

        @pl.when(at_tile // per != core)
        def _():
            out_copy(send_ref, at_slot, at_tile, g).start()

    @pl.when(it >= 2)
    def _():
        out_copy(keep_ref, slot, 0, 0).wait()

    def run(blocks, width_last):
        total = blocks * KB + width_last
        for c in range(parts):
            q = q_ref[c * hc:(c + 1) * hc].reshape(mc, 2 * HD)
            ps = []
            for j in range(blocks + 1):
                width = KB if j < blocks else width_last
                s = lax.dot_general(q, k_scr[g, j * KB:j * KB + width, :], NT, preferred_element_type=F32)
                p = jnp.exp2(s * scale)
                if j == blocks:
                    row = lax.broadcasted_iota(jnp.int32, (hc, TILE, width), 1).reshape(mc, width) + off
                    col = lax.broadcasted_iota(jnp.int32, (mc, width), 1)
                    p = jnp.where(row >= col, p, 0.0)
                ps.append(p.astype(BF16))
            p = jnp.concatenate(ps, axis=1) if len(ps) > 1 else ps[0]
            acc = jnp.dot(p, v_scr[g, :total, :], preferred_element_type=F32)
            den = acc[:, HD:]
            o = (acc[:, :HD] * pltpu.reciprocal(den)).astype(BF16)
            for i in range(hc):
                h = c * hc + i
                o_scr[slot, :, h * HD:(h + 1) * HD] = o[i * TILE:(i + 1) * TILE]
            low_scr[...] = jnp.minimum(low_scr[...], jnp.min(den.reshape(mc // 8, 8, HD), axis=0))

    for blocks in range(seq // KB):
        for half in range(2):
            @pl.when(jnp.logical_and(nfull == blocks, off // 256 == half))
            def _():
                run(blocks, (half + 1) * 256)

    send_out(slot, t)

    def check():
        def redo(step, _):
            tile = step // group
            head = step % group
            cp = pltpu.make_async_copy(q_hbm.at[g * group + head, pl.ds(pl.multiple_of(tile * TILE, TILE), TILE)], qs_scr, sems.at[0])
            cp.start()
            cp.wait()
            q = qs_scr[:, :HD]
            pos = chip * 2 * rows + tile * TILE
            last = pos // TILE
            row = lax.broadcasted_iota(jnp.int32, (TILE, TILE), 0)
            col = lax.broadcasted_iota(jnp.int32, (TILE, TILE), 1)
            m_scr[...] = jnp.full_like(m_scr, -jnp.inf)

            def first(j, _):
                k = k_scr[g, pl.ds(pl.multiple_of(j * TILE, TILE), TILE), :HD]
                s = lax.dot_general(q, k, NT, preferred_element_type=F32)
                s = jnp.where(row + pos >= col + j * TILE, s, -jnp.inf)
                s_scr[j] = s
                m_scr[...] = jnp.maximum(m_scr[...], s)
                return 0

            lax.fori_loop(0, last + 1, first, 0)
            m = jnp.max(m_scr[...], axis=1, keepdims=True)

            def second(j, acc):
                p = jnp.exp2((s_scr[j] - m) * scale).astype(BF16)
                v = v_scr[g, pl.ds(pl.multiple_of(j * TILE, TILE), TILE), :]
                return acc + jnp.dot(p, v, preferred_element_type=F32)

            acc = lax.fori_loop(0, last + 1, second, jnp.zeros((TILE, 2 * HD), F32))
            o = (acc[:, :HD] / acc[:, HD:]).astype(BF16)
            for h in range(group):
                @pl.when(head == h)
                def _():
                    o_scr[slot, :, h * HD:(h + 1) * HD] = o

            @pl.when(head == group - 1)
            def _():
                send_out(slot, tile)
                out_copy(keep_ref, slot, 0, 0).wait()

            return 0

        @pl.when(jnp.min(low_scr[...]) < SMALL)
        def _():
            out_copy(keep_ref, slot, 0, 0).wait()
            out_copy(keep_ref, 1 - slot, 0, 0).wait()
            lax.fori_loop(0, tiles * group, redo, 0)
            o_scr[1 - slot] = o_scr[slot]
            send_out(slot, t)
            send_out(1 - slot, t)

    @pl.when(t == tiles - 1)
    def _():
        check()

    @pl.when(it == tiles * pl.num_programs(0) - 1)
    def _():
        out_copy(keep_ref, slot, 0, 0).wait()
        out_copy(keep_ref, 1 - slot, 0, 0).wait()


def attention(chip, core, q, kv_own, kv_part, kv_same, kv_cross):
    heads, q_rows, _ = q.shape
    rows = q_rows // 2
    seq = 4 * rows
    group = 8
    meta = jnp.stack([chip, core]).astype(jnp.int32)
    out = jax.ShapeDtypeStruct((rows, heads * HD), BF16)
    return pl.pallas_call(
        attn_kernel,
        grid_spec=pltpu.PrefetchScalarGridSpec(
            num_scalar_prefetch=1,
            grid=(heads // group, q_rows // TILE),
            in_specs=[pl.BlockSpec((group, TILE, 2 * HD), lambda g, t, m: (g, t, 0)), ANY, ANY, ANY, ANY, ANY],
            out_specs=[ANY, ANY],
            scratch_shapes=[
                pltpu.VMEM((heads // group, seq, 2 * HD), BF16),
                pltpu.VMEM((heads // group, seq, 2 * HD), BF16),
                pltpu.VMEM((2, TILE, group * HD), BF16),
                pltpu.VMEM((8, HD), F32),
                pltpu.VMEM((TILE, 2 * HD), BF16),
                pltpu.VMEM((seq // TILE, TILE, TILE), F32),
                pltpu.VMEM((TILE, TILE), F32),
                pltpu.SemaphoreType.DMA((8,)),
                pltpu.SemaphoreType.DMA((2,)),
            ],
        ),
        out_shape=[out, out],
        compiler_params=pltpu.CompilerParams(vmem_limit_bytes=VMEM_LIMIT),
        cost_estimate=pl.CostEstimate(flops=4 * heads * q_rows * seq * HD, bytes_accessed=6 * heads * q_rows * HD, transcendentals=0),
        name='attn',
    )(meta, q, q, kv_own, kv_part, kv_same, kv_cross)


def out_kernel(meta, keep_ref, recv_ref, wa_ref, wb_ref, x_ref, o_ref):
    acc = jnp.dot(keep_ref[...], wa_ref[...], preferred_element_type=F32)
    acc += jnp.dot(recv_ref[...], wb_ref[...], preferred_element_type=F32)
    o_ref[...] = (acc + x_ref[...].astype(F32)).astype(BF16)


def out_project(core, keep, recv, w_o, x):
    rows, half = keep.shape
    dim = w_o.shape[1]
    bn = 256
    meta = jnp.stack([core]).astype(jnp.int32)
    full = pl.BlockSpec((rows, half), lambda n, m: (0, 0), pipeline_mode=pl.Buffered(1))
    tile = pl.BlockSpec((rows, bn), lambda n, m: (0, n))
    return pl.pallas_call(
        out_kernel,
        grid_spec=pltpu.PrefetchScalarGridSpec(
            num_scalar_prefetch=1,
            grid=(dim // bn,),
            in_specs=[full, full, pl.BlockSpec((half, bn), lambda n, m: (m[0], n)), pl.BlockSpec((half, bn), lambda n, m: (1 - m[0], n)), tile],
            out_specs=tile,
        ),
        out_shape=jax.ShapeDtypeStruct((rows, dim), BF16),
        compiler_params=pltpu.CompilerParams(vmem_limit_bytes=VMEM_LIMIT),
        cost_estimate=pl.CostEstimate(flops=4 * rows * half * dim, bytes_accessed=4 * half * dim, transcendentals=0),
        name='out_proj',
    )(meta, keep, recv, w_o, w_o, x)


PARTNER = [(0, 1), (1, 0), (2, 3), (3, 2)]


def solution(mesh):
    def device_step(hidden, ln_gain, w_q, w_k, w_v, w_o, q_gain, k_gain):
        rows = hidden.shape[0]
        sp = lax.axis_index('sp')
        chip = sp // 2
        core = sp % 2
        h = rms_norm(hidden, ln_gain)
        h_part = lax.ppermute(h, 'sp', PARTNER)
        cos_k, sin_k = rope_tables(sp * rows + jnp.arange(rows), k_gain)
        cos_q, sin_q = rope_tables(chip * 2 * rows + jnp.arange(2 * rows), q_gain)
        kv_own, kv_other = kv_project(core, h, w_k, w_v, cos_k, sin_k)
        kv_part = lax.ppermute(kv_other, 'sp', PARTNER)
        kv_same = lax.ppermute(kv_own, 'sp', [(0, 2), (1, 3)])
        kv_cross = lax.ppermute(kv_other, 'sp', [(0, 3), (1, 2)])
        q = q_project(core, h, h_part, w_q, cos_q, sin_q)
        keep, send = attention(chip, core, q, kv_own, kv_part, kv_same, kv_cross)
        recv = lax.ppermute(send, 'sp', PARTNER)
        return out_project(core, keep, recv, w_o, hidden)

    row_spec = P(('dp', 'sp'), None)
    return jax.shard_map(device_step, mesh=mesh, in_specs=(row_spec, P(), P(), P(), P(), P(), P(), P()), out_specs=row_spec, check_vma=False)
```

```python
import functools
import math

import jax
import jax.numpy as jnp
from jax import lax
from jax.experimental import pallas as pl
from jax.experimental.pallas import tpu as pltpu
from jax.sharding import PartitionSpec as P

EPS = 1e-6
THETA = 1000000.0
HD = 128
VMEM_LIMIT = 60 * 1024 * 1024
NT = (((1,), (1,)), ((), ()))
F32 = jnp.float32
BF16 = jnp.bfloat16
ANY = pl.BlockSpec(memory_space=pl.ANY)


def rope_tables(positions):
    half = HD // 2
    inv_freq = jnp.power(THETA, -(jnp.arange(half, dtype=F32) * (2.0 / HD)))
    angles = positions.astype(F32)[:, None] * inv_freq[None, :]
    cos = jnp.cos(angles)
    sin = jnp.sin(angles)
    return jnp.concatenate([cos, cos], axis=1), jnp.concatenate([-sin, sin], axis=1)


def front_kernel(x_hbm, g_ref, wq_hbm, wk_hbm, wv_hbm, cos_ref, sin_ref, qg_ref, kg_ref, q_out, k_out, v_out,
                 own_scr, part_scr, w_scr, ka_scr, va_scr, qa_scr, kv_st, q_st,
                 x_sems, w_sems, xs_sems, xr_sems, loc_sems, ps_sems, pr_sems, cs_sems, cr_sems, q_sems):
    sp = lax.axis_index('sp')
    chip = sp // 2
    core = sp % 2
    partner = chip * 2 + 1 - core
    rows, dim = x_hbm.shape
    bn = w_scr.shape[2]
    part_rows = rows // 4
    q_tiles = wq_hbm.shape[1] // 2 // bn

    def weight(src, col, slot):
        return pltpu.make_async_copy(src.at[:, pl.ds(pl.multiple_of(col, bn), bn)], w_scr.at[slot], w_sems.at[slot])

    def k_weight(s, slot):
        return weight(wk_hbm, (2 * core + s) % 4 * bn, slot)

    def v_weight(s, slot):
        return weight(wv_hbm, (2 * core + s) % 4 * bn, slot)

    def q_weight(n):
        return weight(wq_hbm, core * q_tiles * bn + n * bn, n % 4)

    def x_load(i):
        r = pl.ds(i * part_rows, part_rows)
        return pltpu.make_async_copy(x_hbm.at[r], own_scr.at[r], x_sems.at[i])

    def x_send(i):
        r = pl.ds(pl.multiple_of(i * part_rows, part_rows), part_rows)
        return pltpu.make_async_remote_copy(
            src_ref=x_hbm.at[r], dst_ref=part_scr.at[r], send_sem=xs_sems.at[i], recv_sem=xr_sems.at[i],
            device_id={'sp': partner}, device_id_type=pl.DeviceIdType.MESH)

    def norm(ref, i):
        width = 512
        for sub in range(part_rows // 16):
            r = pl.ds(pl.multiple_of(i * part_rows + sub * 16, 16), 16)
            total = None
            for lo in range(0, dim, width):
                x = ref[r, lo:lo + width].astype(F32)
                x = x * x
                for j in range(0, width, HD):
                    total = x[:, j:j + HD] if total is None else total + x[:, j:j + HD]
            inv = lax.rsqrt(jnp.sum(total, axis=1, keepdims=True) * (1.0 / dim) + EPS)
            for lo in range(0, dim, width):
                x = ref[r, lo:lo + width].astype(F32)
                ref[r, lo:lo + width] = (x * inv * g_ref[:, lo:lo + width].astype(F32)).astype(BF16)

    def rope(acc, at, gain_ref):
        var = jnp.mean(acc * acc, axis=-1, keepdims=True)
        t = acc * lax.rsqrt(var + EPS) * gain_ref[...].astype(F32)
        return t * cos_ref[at, :] + pltpu.roll(t, HD // 2, 1) * sin_ref[at, :]

    def kv_multiply(slot):
        ka_scr[...] = jnp.dot(own_scr[...], w_scr[slot], preferred_element_type=F32)
        va_scr[...] = jnp.dot(own_scr[...], w_scr[slot + 1], preferred_element_type=F32)

    def kv_put(s):
        for lo in range(0, rows, 128):
            r = slice(lo, lo + 128)
            for i in range(2):
                cols = slice(i * HD, (i + 1) * HD)
                kv_st[s, 0, i, r, :] = rope(ka_scr[r, cols], r, kg_ref).astype(BF16)
                kv_st[s, 1, i, r, :] = va_scr[r, cols].astype(BF16)

    def q_multiply(slot, lo, src):
        qa_scr[lo:lo + rows, :] = jnp.dot(src[...], w_scr[slot], preferred_element_type=F32)

    def q_put(slot, first):
        for lo in range(first, first + rows, 128):
            r = slice(lo, lo + 128)
            for i in range(bn // HD):
                t = rope(qa_scr[r, i * HD:(i + 1) * HD], r, qg_ref)
                length = jnp.sqrt(jnp.sum(t * t, axis=-1, keepdims=True))
                lane = lax.broadcasted_iota(jnp.int32, t.shape, 1)
                q_st[slot, i, r, :HD] = t.astype(BF16)
                q_st[slot, i, r, HD:] = jnp.where(lane == 0, length, 0.0).astype(BF16)

    def q_store(n, slot):
        return pltpu.make_async_copy(q_st.at[slot], q_out.at[pl.ds(n * (bn // HD), bn // HD)], q_sems.at[slot])

    my_rows = pl.ds(pl.multiple_of(chip * 2 * rows + core * rows, rows), rows)
    outs = (k_out, v_out)

    def local(s, i):
        return pltpu.make_async_copy(kv_st.at[s, i], outs[i].at[pl.ds(2 * s, 2), my_rows], loc_sems.at[s, i])

    def to_partner(s, i):
        return pltpu.make_async_remote_copy(
            src_ref=kv_st.at[s, i], dst_ref=outs[i].at[pl.ds(2 * (s - 2), 2), my_rows],
            send_sem=ps_sems.at[s - 2, i], recv_sem=pr_sems.at[s - 2, i],
            device_id={'sp': partner}, device_id_type=pl.DeviceIdType.MESH)

    def across(s, i):
        other = 2 + (core if s < 2 else 1 - core)
        return pltpu.make_async_remote_copy(
            src_ref=kv_st.at[s, i], dst_ref=outs[i].at[pl.ds(2 * (s % 2), 2), my_rows],
            send_sem=cs_sems.at[s, i], recv_sem=cr_sems.at[core, s % 2, i],
            device_id={'sp': other}, device_id_type=pl.DeviceIdType.MESH)

    def from_across(a, pair, i):
        r = pl.ds(a * rows, rows)
        return pltpu.make_async_remote_copy(
            src_ref=kv_st.at[0, i], dst_ref=outs[i].at[pl.ds(2 * pair, 2), r],
            send_sem=cs_sems.at[0, i], recv_sem=cr_sems.at[a, pair, i],
            device_id={'sp': a}, device_id_type=pl.DeviceIdType.MESH)

    def kv_ship(s):
        for i in range(2):
            (local if s < 2 else to_partner)(s, i).start()

        @pl.when(chip == 0)
        def _():
            for i in range(2):
                across(s, i).start()

    for i in range(4):
        x_load(i).start()
    k_weight(0, 0).start()
    v_weight(0, 1).start()
    barrier = pltpu.get_barrier_semaphore()
    for d in range(1, 4):
        pl.semaphore_signal(barrier, inc=1, device_id={'sp': (sp + d) % 4}, device_id_type=pl.DeviceIdType.MESH)
    pl.semaphore_wait(barrier, 3)
    for i in range(4):
        x_send(i).start()
    k_weight(1, 2).start()
    v_weight(1, 3).start()

    for i in range(4):
        x_load(i).wait()

    def norm_own(i, _):
        norm(own_scr, i)
        return 0

    lax.fori_loop(0, 4, norm_own, 0)
    k_weight(0, 0).wait()
    v_weight(0, 1).wait()
    kv_multiply(0)

    for s in range(1, 4):
        slot = 2 * (s % 2)
        k_weight(s, slot).wait()
        v_weight(s, slot + 1).wait()
        if s < 3:
            k_weight(s + 1, 2 - slot).start()
            v_weight(s + 1, 3 - slot).start()
        else:
            q_weight(0).start()
            q_weight(1).start()
        x_send(s - 1).wait_recv()
        kv_put(s - 1)
        norm(part_scr, s - 1)
        kv_multiply(slot)
        kv_ship(s - 1)

    q_weight(0).wait()
    q_weight(2).start()
    q_weight(3).start()
    x_send(3).wait_recv()
    kv_put(3)
    norm(part_scr, 3)
    q_multiply(0, 0, own_scr)
    q_multiply(0, rows, part_scr)
    kv_ship(3)

    def q_step(n, _):
        q_weight(n).wait()

        @pl.when(n + 3 < q_tiles)
        def _():
            q_weight(n + 3).start()

        slot = (n + 1) % 2

        @pl.when(n >= 3)
        def _():
            q_store(n - 3, slot).wait()

        q_put(slot, 0)
        q_multiply(n % 4, 0, own_scr)
        q_put(slot, rows)
        q_multiply(n % 4, rows, part_scr)
        q_store(n - 1, slot).start()
        return 0

    lax.fori_loop(1, q_tiles, q_step, 0)
    slot = (q_tiles - 1) % 2
    q_store(q_tiles - 3, slot).wait()
    q_put(slot, 0)
    q_put(slot, rows)
    q_store(q_tiles - 1, slot).start()

    for i in range(4):
        x_send(i).wait_send()
    for s in range(2):
        for i in range(2):
            local(s, i).wait()
            to_partner(s + 2, i).wait()

    @pl.when(chip == 0)
    def _():
        for s in range(4):
            for i in range(2):
                across(s, i).wait_send()

    @pl.when(chip == 1)
    def _():
        for a in range(2):
            for pair in range(2):
                for i in range(2):
                    from_across(a, pair, i).wait_recv()

    q_store(q_tiles - 2, 1 - slot).wait()
    q_store(q_tiles - 1, slot).wait()


def front(x, gain, w_q, w_k, w_v, cos, sin, q_gain, k_gain):
    rows, dim = x.shape
    bn = 256
    heads = w_q.shape[1] // HD // 2
    kv_heads = w_k.shape[1] // HD // 2
    vmem = pl.BlockSpec(memory_space=pltpu.VMEM)
    kv = jax.ShapeDtypeStruct((kv_heads, 4 * rows, HD), BF16)
    dma = pltpu.SemaphoreType.DMA
    return pl.pallas_call(
        front_kernel,
        in_specs=[ANY, vmem, ANY, ANY, ANY, vmem, vmem, vmem, vmem],
        out_specs=[ANY, ANY, ANY],
        out_shape=[jax.ShapeDtypeStruct((heads, 2 * rows, 2 * HD), BF16), kv, kv],
        scratch_shapes=[
            pltpu.VMEM((rows, dim), BF16),
            pltpu.VMEM((rows, dim), BF16),
            pltpu.VMEM((4, dim, bn), BF16),
            pltpu.VMEM((rows, bn), F32),
            pltpu.VMEM((rows, bn), F32),
            pltpu.VMEM((2 * rows, bn), F32),
            pltpu.VMEM((4, 2, 2, rows, HD), BF16),
            pltpu.VMEM((2, bn // HD, 2 * rows, 2 * HD), BF16),
            dma((4,)), dma((4,)), dma((4,)), dma((4,)), dma((2, 2)), dma((2, 2)), dma((2, 2)), dma((4, 2)), dma((2, 2, 2)), dma((2,)),
        ],
        compiler_params=pltpu.CompilerParams(vmem_limit_bytes=VMEM_LIMIT, collective_id=0, has_side_effects=True),
        cost_estimate=pl.CostEstimate(flops=2 * rows * dim * (w_q.shape[1] + 2 * w_k.shape[1]), bytes_accessed=dim * w_q.shape[1], transcendentals=0),
        name='front',
    )(x, gain.reshape(1, dim), w_q, w_k, w_v, cos, sin, q_gain.reshape(1, HD), k_gain.reshape(1, HD))


TILE = 128
KB = 512
SMALL = 2.0 ** -90


def attn_kernel(meta, q_ref, q_hbm, k_hbm, v_hbm, keep_ref, send_ref, k_scr, v_scr, o_scr, low_scr, qs_scr, s_scr, m_scr, sems, o_sems):
    g = pl.program_id(0)
    t = pl.program_id(1)
    tiles = pl.num_programs(1)
    chip = meta[0]
    core = meta[1]
    rows = k_hbm.shape[1] // 4
    group = q_ref.shape[0]
    seq = k_scr.shape[1]
    scale = HD ** -0.5 * math.log2(math.e)
    per = rows // TILE

    def base(tile):
        return (chip * 2 + jnp.where(tile < per, core, 1 - core)) * rows + tile % per * TILE

    @pl.when(jnp.logical_and(g == 0, t == 0))
    def _():
        for x in range(2):
            @pl.when(chip == x)
            def _():
                span = pl.ds(0, 2 * (x + 1) * rows)
                cps = [
                    pltpu.make_async_copy(src.at[:, span], dst.at[:, span, pl.ds(0, HD)], sems.at[i])
                    for i, (src, dst) in enumerate(((k_hbm, k_scr), (v_hbm, v_scr)))
                ]
                for cp in cps:
                    cp.start()
                if x == 0:
                    k_scr[:, 2 * rows:, :HD] = jnp.zeros((k_scr.shape[0], 2 * rows, HD), BF16)
                v_scr[:, :, HD:] = jnp.ones((v_scr.shape[0], seq, HD), BF16)
                for cp in cps:
                    cp.wait()

    @pl.when(t == 0)
    def _():
        k = k_scr[g, :, :HD]
        sums = jnp.dot(k * k, jnp.ones((HD, HD), BF16), preferred_element_type=F32)
        longest = jnp.sqrt(jnp.max(sums)) * 1.02
        lane = lax.broadcasted_iota(jnp.int32, (seq, HD), 1)
        k_scr[g, :, HD:] = jnp.where(lane == 0, -longest, 0.0).astype(BF16)
        low_scr[...] = jnp.ones_like(low_scr)

    pos0 = base(t)
    nfull = pos0 // KB
    off = pos0 - nfull * KB
    parts = 2
    hc = group // parts
    mc = hc * TILE

    it = g * tiles + t
    slot = it % 2

    def out_copy(ref, at_slot, at_tile, at_group):
        rows_at = pl.ds(pl.multiple_of((at_tile % per) * TILE, TILE), TILE)
        cols_at = pl.ds(pl.multiple_of(at_group * group * HD, group * HD), group * HD)
        return pltpu.make_async_copy(o_scr.at[at_slot], ref.at[rows_at, cols_at], o_sems.at[at_slot])

    def send_out(at_slot, at_tile):
        @pl.when(at_tile < per)
        def _():
            out_copy(keep_ref, at_slot, at_tile, g).start()

        @pl.when(at_tile >= per)
        def _():
            out_copy(send_ref, at_slot, at_tile, g).start()

    @pl.when(it >= 2)
    def _():
        out_copy(keep_ref, slot, 0, 0).wait()

    def run(blocks, width_last):
        total = blocks * KB + width_last
        for c in range(parts):
            q = q_ref[c * hc:(c + 1) * hc].reshape(mc, 2 * HD)
            ps = []
            for j in range(blocks + 1):
                width = KB if j < blocks else width_last
                s = lax.dot_general(q, k_scr[g, j * KB:j * KB + width, :], NT, preferred_element_type=F32)
                p = jnp.exp2(s * scale)
                if j == blocks:
                    row = lax.broadcasted_iota(jnp.int32, (hc, TILE, width), 1).reshape(mc, width) + off
                    col = lax.broadcasted_iota(jnp.int32, (mc, width), 1)
                    p = jnp.where(row >= col, p, 0.0)
                ps.append(p.astype(BF16))
            p = jnp.concatenate(ps, axis=1) if len(ps) > 1 else ps[0]
            acc = jnp.dot(p, v_scr[g, :total, :], preferred_element_type=F32)
            den = acc[:, HD:]
            o = (acc[:, :HD] * pltpu.reciprocal(den)).astype(BF16)
            for i in range(hc):
                h = c * hc + i
                o_scr[slot, :, h * HD:(h + 1) * HD] = o[i * TILE:(i + 1) * TILE]
            low_scr[...] = jnp.minimum(low_scr[...], jnp.min(den.reshape(mc // 8, 8, HD), axis=0))

    for blocks in range(seq // KB):
        for half in range(2):
            @pl.when(jnp.logical_and(nfull == blocks, off // 256 == half))
            def _():
                run(blocks, (half + 1) * 256)

    send_out(slot, t)

    def check():
        def redo(step, _):
            tile = step // group
            head = step % group
            cp = pltpu.make_async_copy(q_hbm.at[g * group + head, pl.ds(pl.multiple_of(tile * TILE, TILE), TILE)], qs_scr, sems.at[0])
            cp.start()
            cp.wait()
            q = qs_scr[:, :HD]
            pos = base(tile)
            last = pos // TILE
            row = lax.broadcasted_iota(jnp.int32, (TILE, TILE), 0)
            col = lax.broadcasted_iota(jnp.int32, (TILE, TILE), 1)
            m_scr[...] = jnp.full_like(m_scr, -jnp.inf)

            def first(j, _):
                k = k_scr[g, pl.ds(pl.multiple_of(j * TILE, TILE), TILE), :HD]
                s = lax.dot_general(q, k, NT, preferred_element_type=F32)
                s = jnp.where(row + pos >= col + j * TILE, s, -jnp.inf)
                s_scr[j] = s
                m_scr[...] = jnp.maximum(m_scr[...], s)
                return 0

            lax.fori_loop(0, last + 1, first, 0)
            m = jnp.max(m_scr[...], axis=1, keepdims=True)

            def second(j, acc):
                p = jnp.exp2((s_scr[j] - m) * scale).astype(BF16)
                v = v_scr[g, pl.ds(pl.multiple_of(j * TILE, TILE), TILE), :]
                return acc + jnp.dot(p, v, preferred_element_type=F32)

            acc = lax.fori_loop(0, last + 1, second, jnp.zeros((TILE, 2 * HD), F32))
            o = (acc[:, :HD] / acc[:, HD:]).astype(BF16)
            for h in range(group):
                @pl.when(head == h)
                def _():
                    o_scr[slot, :, h * HD:(h + 1) * HD] = o

            @pl.when(head == group - 1)
            def _():
                send_out(slot, tile)
                out_copy(keep_ref, slot, 0, 0).wait()

            return 0

        @pl.when(jnp.min(low_scr[...]) < SMALL)
        def _():
            out_copy(keep_ref, slot, 0, 0).wait()
            out_copy(keep_ref, 1 - slot, 0, 0).wait()
            lax.fori_loop(0, tiles * group, redo, 0)
            o_scr[1 - slot] = o_scr[slot]
            send_out(slot, t)
            send_out(1 - slot, t)

    @pl.when(t == tiles - 1)
    def _():
        check()

    @pl.when(it == tiles * pl.num_programs(0) - 1)
    def _():
        out_copy(keep_ref, slot, 0, 0).wait()
        out_copy(keep_ref, 1 - slot, 0, 0).wait()


def attention(chip, core, q, k, v):
    heads, q_rows, _ = q.shape
    rows = q_rows // 2
    seq = 4 * rows
    group = 8
    meta = jnp.stack([chip, core]).astype(jnp.int32)
    out = jax.ShapeDtypeStruct((rows, heads * HD), BF16)
    return pl.pallas_call(
        attn_kernel,
        grid_spec=pltpu.PrefetchScalarGridSpec(
            num_scalar_prefetch=1,
            grid=(heads // group, q_rows // TILE),
            in_specs=[pl.BlockSpec((group, TILE, 2 * HD), lambda g, t, m: (g, t, 0)), ANY, ANY, ANY],
            out_specs=[ANY, ANY],
            scratch_shapes=[
                pltpu.VMEM((heads // group, seq, 2 * HD), BF16),
                pltpu.VMEM((heads // group, seq, 2 * HD), BF16),
                pltpu.VMEM((2, TILE, group * HD), BF16),
                pltpu.VMEM((8, HD), F32),
                pltpu.VMEM((TILE, 2 * HD), BF16),
                pltpu.VMEM((seq // TILE, TILE, TILE), F32),
                pltpu.VMEM((TILE, TILE), F32),
                pltpu.SemaphoreType.DMA((2,)),
                pltpu.SemaphoreType.DMA((2,)),
            ],
        ),
        out_shape=[out, out],
        compiler_params=pltpu.CompilerParams(vmem_limit_bytes=VMEM_LIMIT),
        cost_estimate=pl.CostEstimate(flops=4 * heads * q_rows * seq * HD, bytes_accessed=6 * heads * q_rows * HD, transcendentals=0),
        name='attn',
    )(meta, q, q, k, v)


def out_kernel(meta, keep_ref, recv_ref, wa_ref, wb_ref, x_ref, o_ref):
    acc = jnp.dot(keep_ref[...], wa_ref[...], preferred_element_type=F32)
    acc += jnp.dot(recv_ref[...], wb_ref[...], preferred_element_type=F32)
    o_ref[...] = (acc + x_ref[...].astype(F32)).astype(BF16)


def out_project(core, keep, recv, w_o, x):
    rows, half = keep.shape
    dim = w_o.shape[1]
    bn = 256
    meta = jnp.stack([core]).astype(jnp.int32)
    full = pl.BlockSpec((rows, half), lambda n, m: (0, 0), pipeline_mode=pl.Buffered(1))
    tile = pl.BlockSpec((rows, bn), lambda n, m: (0, n))
    return pl.pallas_call(
        out_kernel,
        grid_spec=pltpu.PrefetchScalarGridSpec(
            num_scalar_prefetch=1,
            grid=(dim // bn,),
            in_specs=[full, full, pl.BlockSpec((half, bn), lambda n, m: (m[0], n)), pl.BlockSpec((half, bn), lambda n, m: (1 - m[0], n)), tile],
            out_specs=tile,
        ),
        out_shape=jax.ShapeDtypeStruct((rows, dim), BF16),
        compiler_params=pltpu.CompilerParams(vmem_limit_bytes=VMEM_LIMIT),
        cost_estimate=pl.CostEstimate(flops=4 * rows * half * dim, bytes_accessed=4 * half * dim, transcendentals=0),
        name='out_proj',
    )(meta, keep, recv, w_o, w_o, x)


PARTNER = [(0, 1), (1, 0), (2, 3), (3, 2)]


def solution(mesh):
    def device_step(hidden, ln_gain, w_q, w_k, w_v, w_o, q_gain, k_gain):
        rows = hidden.shape[0]
        sp = lax.axis_index('sp')
        chip = sp // 2
        core = sp % 2
        mine = jnp.arange(rows)
        positions = chip * 2 * rows + jnp.concatenate([core * rows + mine, (1 - core) * rows + mine])
        cos, sin = rope_tables(positions)
        q, k, v = front(hidden, ln_gain, w_q, w_k, w_v, cos, sin, q_gain, k_gain)
        keep, send = attention(chip, core, q, k, v)
        recv = lax.ppermute(send, 'sp', PARTNER)
        return out_project(core, keep, recv, w_o, hidden)

    row_spec = P(('dp', 'sp'), None)
    return jax.shard_map(device_step, mesh=mesh, in_specs=(row_spec, P(), P(), P(), P(), P(), P(), P()), out_specs=row_spec, check_vma=False)
```

```python
import functools
import math

import jax
import jax.numpy as jnp
import numpy as np
from jax import lax
from jax.experimental import pallas as pl
from jax.experimental.pallas import tpu as pltpu
from jax.sharding import PartitionSpec as P

EPS = 1e-6
THETA = 1000000.0
HD = 128
VMEM_LIMIT = 60 * 1024 * 1024
NT = (((1,), (1,)), ((), ()))
F32 = jnp.float32
BF16 = jnp.bfloat16
ANY = pl.BlockSpec(memory_space=pl.ANY)


STRIDE = 64


def rope_parts(seq):
    half = HD // 2
    inv_freq = THETA ** -(np.arange(half) * (2.0 / HD))
    parts = []
    for positions in (np.arange(0, seq, STRIDE), np.arange(STRIDE)):
        angles = positions[:, None] * inv_freq[None, :]
        parts.append(np.concatenate([np.cos(angles), np.cos(angles)], axis=1))
        parts.append(np.concatenate([-np.sin(angles), np.sin(angles)], axis=1))
    return np.concatenate(parts, axis=0).astype(np.float32)


def front_kernel(x_hbm, gain_ref, wq_hbm, wk_hbm, wv_hbm, tab_ref, qgain_ref, kgain_ref, q_out, k_out, v_out,
                 g_ref, qg_ref, kg_ref, cos_ref, sin_ref, own_scr, part_scr, w_scr, ka_scr, va_scr, qa_scr, kv_st, q_st,
                 x_sems, w_sems, xs_sems, xr_sems, loc_sems, ps_sems, pr_sems, cs_sems, cr_sems, q_sems):
    sp = lax.axis_index('sp')
    chip = sp // 2
    core = sp % 2
    partner = chip * 2 + 1 - core
    rows, dim = x_hbm.shape
    bn = w_scr.shape[2]
    part_rows = rows // 4
    q_tiles = wq_hbm.shape[1] // 2 // bn

    def weight(src, col, slot):
        return pltpu.make_async_copy(src.at[:, pl.ds(pl.multiple_of(col, bn), bn)], w_scr.at[slot], w_sems.at[slot])

    def k_weight(s, slot):
        return weight(wk_hbm, (2 * core + s) % 4 * bn, slot)

    def v_weight(s, slot):
        return weight(wv_hbm, (2 * core + s) % 4 * bn, slot)

    def q_weight(n):
        return weight(wq_hbm, core * q_tiles * bn + n * bn, n % 4)

    def x_load(i):
        r = pl.ds(i * part_rows, part_rows)
        return pltpu.make_async_copy(x_hbm.at[r], own_scr.at[r], x_sems.at[i])

    def x_send(i):
        r = pl.ds(pl.multiple_of(i * part_rows, part_rows), part_rows)
        return pltpu.make_async_remote_copy(
            src_ref=x_hbm.at[r], dst_ref=part_scr.at[r], send_sem=xs_sems.at[i], recv_sem=xr_sems.at[i],
            device_id={'sp': partner}, device_id_type=pl.DeviceIdType.MESH)

    def norm(ref, i):
        width = 512
        for sub in range(part_rows // 16):
            r = pl.ds(pl.multiple_of(i * part_rows + sub * 16, 16), 16)
            total = None
            for lo in range(0, dim, width):
                x = ref[r, lo:lo + width].astype(F32)
                x = x * x
                for j in range(0, width, HD):
                    total = x[:, j:j + HD] if total is None else total + x[:, j:j + HD]
            inv = lax.rsqrt(jnp.sum(total, axis=1, keepdims=True) * (1.0 / dim) + EPS)
            for lo in range(0, dim, width):
                x = ref[r, lo:lo + width].astype(F32)
                ref[r, lo:lo + width] = (x * inv * g_ref[:, lo:lo + width]).astype(BF16)

    def rope(acc, at, gain):
        var = jnp.mean(acc * acc, axis=-1, keepdims=True)
        t = acc * lax.rsqrt(var + EPS) * gain[...]
        return t * cos_ref[at, :] + pltpu.roll(t, HD // 2, 1) * sin_ref[at, :]

    def kv_multiply(slot):
        ka_scr[...] = jnp.dot(own_scr[...], w_scr[slot], preferred_element_type=F32)
        va_scr[...] = jnp.dot(own_scr[...], w_scr[slot + 1], preferred_element_type=F32)

    def kv_put(s):
        for lo in range(0, rows, 128):
            r = slice(lo, lo + 128)
            for i in range(2):
                cols = slice(i * HD, (i + 1) * HD)
                kv_st[s, 0, i, r, :] = rope(ka_scr[r, cols], r, kg_ref).astype(BF16)
                kv_st[s, 1, i, r, :] = va_scr[r, cols].astype(BF16)

    def q_multiply(slot, lo, src):
        qa_scr[lo:lo + rows, :] = jnp.dot(src[...], w_scr[slot], preferred_element_type=F32)

    def q_put(slot, first):
        for lo in range(first, first + rows, 128):
            r = slice(lo, lo + 128)
            for i in range(bn // HD):
                t = rope(qa_scr[r, i * HD:(i + 1) * HD], r, qg_ref)
                length = jnp.sqrt(jnp.sum(t * t, axis=-1, keepdims=True))
                lane = lax.broadcasted_iota(jnp.int32, t.shape, 1)
                q_st[slot, i, r, :HD] = t.astype(BF16)
                q_st[slot, i, r, HD:] = jnp.where(lane == 0, length, 0.0).astype(BF16)

    def q_store(n, slot):
        return pltpu.make_async_copy(q_st.at[slot], q_out.at[pl.ds(n * (bn // HD), bn // HD)], q_sems.at[slot])

    my_rows = pl.ds(pl.multiple_of(chip * 2 * rows + core * rows, rows), rows)
    outs = (k_out, v_out)

    def local(s, i):
        return pltpu.make_async_copy(kv_st.at[s, i], outs[i].at[pl.ds(2 * s, 2), my_rows], loc_sems.at[s, i])

    def to_partner(s, i):
        return pltpu.make_async_remote_copy(
            src_ref=kv_st.at[s, i], dst_ref=outs[i].at[pl.ds(2 * (s - 2), 2), my_rows],
            send_sem=ps_sems.at[s - 2, i], recv_sem=pr_sems.at[s - 2, i],
            device_id={'sp': partner}, device_id_type=pl.DeviceIdType.MESH)

    def across(s, i):
        other = 2 + (core if s < 2 else 1 - core)
        return pltpu.make_async_remote_copy(
            src_ref=kv_st.at[s, i], dst_ref=outs[i].at[pl.ds(2 * (s % 2), 2), my_rows],
            send_sem=cs_sems.at[s, i], recv_sem=cr_sems.at[core, s % 2, i],
            device_id={'sp': other}, device_id_type=pl.DeviceIdType.MESH)

    def from_across(a, pair, i):
        r = pl.ds(a * rows, rows)
        return pltpu.make_async_remote_copy(
            src_ref=kv_st.at[0, i], dst_ref=outs[i].at[pl.ds(2 * pair, 2), r],
            send_sem=cs_sems.at[0, i], recv_sem=cr_sems.at[a, pair, i],
            device_id={'sp': a}, device_id_type=pl.DeviceIdType.MESH)

    def kv_ship(s):
        for i in range(2):
            (local if s < 2 else to_partner)(s, i).start()

        @pl.when(chip == 0)
        def _():
            for i in range(2):
                across(s, i).start()

    for i in range(4):
        x_load(i).start()
    k_weight(0, 0).start()
    v_weight(0, 1).start()
    barrier = pltpu.get_barrier_semaphore()
    for d in range(1, 4):
        pl.semaphore_signal(barrier, inc=1, device_id={'sp': (sp + d) % 4}, device_id_type=pl.DeviceIdType.MESH)
    pl.semaphore_wait(barrier, 3)
    for i in range(4):
        x_send(i).start()
    k_weight(1, 2).start()
    v_weight(1, 3).start()

    g_ref[...] = gain_ref[...].astype(F32).reshape(1, dim)
    qg_ref[...] = qgain_ref[...].astype(F32).reshape(1, HD)
    kg_ref[...] = kgain_ref[...].astype(F32).reshape(1, HD)
    coarse = 4 * rows // STRIDE
    cos_b = tab_ref[2 * coarse:2 * coarse + STRIDE, :]
    sin_b = tab_ref[2 * coarse + STRIDE:, :]
    for j in range(2 * rows // STRIDE):
        side = core if j * STRIDE < rows else 1 - core
        a = (chip * 2 + side) * (rows // STRIDE) + j % (rows // STRIDE)
        cos_a = tab_ref[pl.ds(a, 1), :]
        sin_a = tab_ref[pl.ds(coarse + a, 1), :]
        r = slice(j * STRIDE, (j + 1) * STRIDE)
        cos_ref[r, :] = cos_a * cos_b - sin_a * sin_b
        sin_ref[r, :] = sin_a * cos_b + cos_a * sin_b

    for i in range(4):
        x_load(i).wait()

    def norm_own(i, _):
        norm(own_scr, i)
        return 0

    lax.fori_loop(0, 4, norm_own, 0)
    k_weight(0, 0).wait()
    v_weight(0, 1).wait()
    kv_multiply(0)

    for s in range(1, 4):
        slot = 2 * (s % 2)
        k_weight(s, slot).wait()
        v_weight(s, slot + 1).wait()
        if s < 3:
            k_weight(s + 1, 2 - slot).start()
            v_weight(s + 1, 3 - slot).start()
        else:
            q_weight(0).start()
            q_weight(1).start()
        x_send(s - 1).wait_recv()
        kv_put(s - 1)
        norm(part_scr, s - 1)
        kv_multiply(slot)
        kv_ship(s - 1)

    q_weight(0).wait()
    q_weight(2).start()
    q_weight(3).start()
    x_send(3).wait_recv()
    kv_put(3)
    norm(part_scr, 3)
    q_multiply(0, 0, own_scr)
    q_multiply(0, rows, part_scr)
    kv_ship(3)

    def q_step(n, _):
        q_weight(n).wait()

        @pl.when(n + 3 < q_tiles)
        def _():
            q_weight(n + 3).start()

        slot = (n + 1) % 2

        @pl.when(n >= 3)
        def _():
            q_store(n - 3, slot).wait()

        q_put(slot, 0)
        q_multiply(n % 4, 0, own_scr)
        q_put(slot, rows)
        q_multiply(n % 4, rows, part_scr)
        q_store(n - 1, slot).start()
        return 0

    lax.fori_loop(1, q_tiles, q_step, 0)
    slot = (q_tiles - 1) % 2
    q_store(q_tiles - 3, slot).wait()
    q_put(slot, 0)
    q_put(slot, rows)
    q_store(q_tiles - 1, slot).start()

    for i in range(4):
        x_send(i).wait_send()
    for s in range(2):
        for i in range(2):
            local(s, i).wait()
            to_partner(s + 2, i).wait()

    @pl.when(chip == 0)
    def _():
        for s in range(4):
            for i in range(2):
                across(s, i).wait_send()

    @pl.when(chip == 1)
    def _():
        for a in range(2):
            for pair in range(2):
                for i in range(2):
                    from_across(a, pair, i).wait_recv()

    q_store(q_tiles - 2, 1 - slot).wait()
    q_store(q_tiles - 1, slot).wait()


def front(x, gain, w_q, w_k, w_v, q_gain, k_gain):
    rows, dim = x.shape
    bn = 256
    heads = w_q.shape[1] // HD // 2
    kv_heads = w_k.shape[1] // HD // 2
    vmem = pl.BlockSpec(memory_space=pltpu.VMEM)
    kv = jax.ShapeDtypeStruct((kv_heads, 4 * rows, HD), BF16)
    dma = pltpu.SemaphoreType.DMA
    return pl.pallas_call(
        front_kernel,
        in_specs=[ANY, vmem, ANY, ANY, ANY, vmem, vmem, vmem],
        out_specs=[ANY, ANY, ANY],
        out_shape=[jax.ShapeDtypeStruct((heads, 2 * rows, 2 * HD), BF16), kv, kv],
        scratch_shapes=[
            pltpu.VMEM((1, dim), F32),
            pltpu.VMEM((1, HD), F32),
            pltpu.VMEM((1, HD), F32),
            pltpu.VMEM((2 * rows, HD), F32),
            pltpu.VMEM((2 * rows, HD), F32),
            pltpu.VMEM((rows, dim), BF16),
            pltpu.VMEM((rows, dim), BF16),
            pltpu.VMEM((4, dim, bn), BF16),
            pltpu.VMEM((rows, bn), F32),
            pltpu.VMEM((rows, bn), F32),
            pltpu.VMEM((2 * rows, bn), F32),
            pltpu.VMEM((4, 2, 2, rows, HD), BF16),
            pltpu.VMEM((2, bn // HD, 2 * rows, 2 * HD), BF16),
            dma((4,)), dma((4,)), dma((4,)), dma((4,)), dma((2, 2)), dma((2, 2)), dma((2, 2)), dma((4, 2)), dma((2, 2, 2)), dma((2,)),
        ],
        compiler_params=pltpu.CompilerParams(vmem_limit_bytes=VMEM_LIMIT, collective_id=0, has_side_effects=True),
        cost_estimate=pl.CostEstimate(flops=2 * rows * dim * (w_q.shape[1] + 2 * w_k.shape[1]), bytes_accessed=dim * w_q.shape[1], transcendentals=0),
        name='front',
    )(x, gain, w_q, w_k, w_v, jnp.asarray(rope_parts(4 * rows)), q_gain, k_gain)


TILE = 128
KB = 512
SMALL = 2.0 ** -90


def attn_kernel(q_hbm, k_hbm, v_hbm, keep_ref, send_ref, q_scr, k_scr, v_scr, o_scr, low_scr, s_scr, m_scr, q_sems, k_sems, v_sems, o_sems):
    sp = lax.axis_index('sp')
    chip = sp // 2
    core = sp % 2
    groups, seq, _ = k_hbm.shape
    rows = seq // 4
    group = q_scr.shape[0] // groups
    tiles = 2 * rows // TILE
    per = rows // TILE
    scale = HD ** -0.5 * math.log2(math.e)

    def base(tile):
        return (chip * 2 + jnp.where(tile < per, core, 1 - core)) * rows + tile % per * TILE

    def kv_load(g, x):
        span = pl.ds(0, 2 * (x + 1) * rows)
        return [
            pltpu.make_async_copy(src.at[g, span], dst.at[g, span, pl.ds(0, HD)], sems.at[g])
            for src, dst, sems in ((k_hbm, k_scr, k_sems), (v_hbm, v_scr, v_sems))
        ]

    def q_load(t):
        r = pl.ds(t * TILE, TILE)
        return pltpu.make_async_copy(q_hbm.at[:, r], q_scr.at[:, r], q_sems.at[t])

    def kv_start(g):
        for x in range(2):
            @pl.when(chip == x)
            def _():
                for cp in kv_load(g, x):
                    cp.start()

    def kv_wait(g):
        for x in range(2):
            @pl.when(chip == x)
            def _():
                for cp in kv_load(g, x):
                    cp.wait()

    kv_start(0)
    q_load(0).start()
    for g in range(1, groups):
        kv_start(g)
    for t in range(1, tiles):
        q_load(t).start()

    @pl.when(chip == 0)
    def _():
        k_scr[:, 2 * rows:, :HD] = jnp.zeros((groups, 2 * rows, HD), BF16)

    v_scr[:, :, HD:] = jnp.ones((groups, seq, HD), BF16)

    def open_group(g):
        kv_wait(g)
        k = k_scr[g, :, :HD]
        sums = jnp.dot(k * k, jnp.ones((HD, HD), BF16), preferred_element_type=F32)
        longest = jnp.sqrt(jnp.max(sums)) * 1.02
        lane = lax.broadcasted_iota(jnp.int32, (seq, HD), 1)
        k_scr[g, :, HD:] = jnp.where(lane == 0, -longest, 0.0).astype(BF16)
        low_scr[g] = jnp.ones((8, HD), F32)

    def out_copy(ref, slot, tile, g):
        rows_at = pl.ds(pl.multiple_of((tile % per) * TILE, TILE), TILE)
        cols_at = pl.ds(pl.multiple_of(g * group * HD, group * HD), group * HD)
        return pltpu.make_async_copy(o_scr.at[slot], ref.at[rows_at, cols_at], o_sems.at[slot])

    def send_out(slot, tile, g):
        @pl.when(tile < per)
        def _():
            out_copy(keep_ref, slot, tile, g).start()

        @pl.when(tile >= per)
        def _():
            out_copy(send_ref, slot, tile, g).start()

    parts = 2
    hc = group // parts
    mc = hc * TILE

    def run(g, t, slot, off, blocks, width_last):
        total = blocks * KB + width_last
        at = pl.ds(pl.multiple_of(t * TILE, TILE), TILE)
        for c in range(parts):
            q = q_scr[pl.ds(g * group + c * hc, hc), at, :].reshape(mc, 2 * HD)
            ps = []
            for j in range(blocks + 1):
                width = KB if j < blocks else width_last
                s = lax.dot_general(q, k_scr[g, j * KB:j * KB + width, :], NT, preferred_element_type=F32)
                p = jnp.exp2(s * scale)
                if j == blocks:
                    row = lax.broadcasted_iota(jnp.int32, (hc, TILE, width), 1).reshape(mc, width) + off
                    col = lax.broadcasted_iota(jnp.int32, (mc, width), 1)
                    p = jnp.where(row >= col, p, 0.0)
                ps.append(p.astype(BF16))
            p = jnp.concatenate(ps, axis=1) if len(ps) > 1 else ps[0]
            acc = jnp.dot(p, v_scr[g, :total, :], preferred_element_type=F32)
            den = acc[:, HD:]
            o = (acc[:, :HD] * pltpu.reciprocal(den)).astype(BF16)
            for i in range(hc):
                h = c * hc + i
                o_scr[slot, :, h * HD:(h + 1) * HD] = o[i * TILE:(i + 1) * TILE]
            low_scr[g] = jnp.minimum(low_scr[g], jnp.min(den.reshape(mc // 8, 8, HD), axis=0))

    def redo(g, slot):
        def one(step, _):
            tile = step // group
            head = step % group
            q = q_scr[g * group + head, pl.ds(pl.multiple_of(tile * TILE, TILE), TILE), :HD]
            pos = base(tile)
            last = pos // TILE
            row = lax.broadcasted_iota(jnp.int32, (TILE, TILE), 0)
            col = lax.broadcasted_iota(jnp.int32, (TILE, TILE), 1)
            m_scr[...] = jnp.full_like(m_scr, -jnp.inf)

            def first(j, _):
                k = k_scr[g, pl.ds(pl.multiple_of(j * TILE, TILE), TILE), :HD]
                s = lax.dot_general(q, k, NT, preferred_element_type=F32)
                s = jnp.where(row + pos >= col + j * TILE, s, -jnp.inf)
                s_scr[j] = s
                m_scr[...] = jnp.maximum(m_scr[...], s)
                return 0

            lax.fori_loop(0, last + 1, first, 0)
            m = jnp.max(m_scr[...], axis=1, keepdims=True)

            def second(j, acc):
                p = jnp.exp2((s_scr[j] - m) * scale).astype(BF16)
                v = v_scr[g, pl.ds(pl.multiple_of(j * TILE, TILE), TILE), :]
                return acc + jnp.dot(p, v, preferred_element_type=F32)

            acc = lax.fori_loop(0, last + 1, second, jnp.zeros((TILE, 2 * HD), F32))
            o = (acc[:, :HD] / acc[:, HD:]).astype(BF16)
            for h in range(group):
                @pl.when(head == h)
                def _():
                    o_scr[slot, :, h * HD:(h + 1) * HD] = o

            @pl.when(head == group - 1)
            def _():
                send_out(slot, tile, g)
                out_copy(keep_ref, slot, 0, 0).wait()

            return 0

        lax.fori_loop(0, tiles * group, one, 0)

    def step(it, _):
        t = it // groups
        g = it % groups
        slot = it % 2

        @pl.when(g == 0)
        def _():
            q_load(t).wait()

        @pl.when(t == 0)
        def _():
            open_group(g)

        @pl.when(it >= 2)
        def _():
            out_copy(keep_ref, slot, 0, 0).wait()

        pos0 = base(t)
        nfull = pos0 // KB
        off = pos0 - nfull * KB
        for blocks in range(seq // KB):
            for half in range(2):
                @pl.when(jnp.logical_and(nfull == blocks, off // 256 == half))
                def _():
                    run(g, t, slot, off, blocks, (half + 1) * 256)

        send_out(slot, t, g)
        return 0

    lax.fori_loop(0, groups * tiles, step, 0)
    for slot in range(2):
        out_copy(keep_ref, slot, 0, 0).wait()

    @pl.when(jnp.min(low_scr[...]) < SMALL)
    def _():
        def group_again(g, _):
            redo(g, 0)
            return 0

        lax.fori_loop(0, groups, group_again, 0)


def attention(q, k, v):
    heads, q_rows, _ = q.shape
    groups, seq, _ = k.shape
    group = heads // groups
    out = jax.ShapeDtypeStruct((q_rows // 2, heads * HD), BF16)
    dma = pltpu.SemaphoreType.DMA
    return pl.pallas_call(
        attn_kernel,
        in_specs=[ANY, ANY, ANY],
        out_specs=[ANY, ANY],
        scratch_shapes=[
            pltpu.VMEM((heads, q_rows, 2 * HD), BF16),
            pltpu.VMEM((groups, seq, 2 * HD), BF16),
            pltpu.VMEM((groups, seq, 2 * HD), BF16),
            pltpu.VMEM((2, TILE, group * HD), BF16),
            pltpu.VMEM((groups, 8, HD), F32),
            pltpu.VMEM((seq // TILE, TILE, TILE), F32),
            pltpu.VMEM((TILE, TILE), F32),
            dma((q_rows // TILE,)), dma((groups,)), dma((groups,)), dma((2,)),
        ],
        out_shape=[out, out],
        compiler_params=pltpu.CompilerParams(vmem_limit_bytes=VMEM_LIMIT),
        cost_estimate=pl.CostEstimate(flops=4 * heads * q_rows * seq * HD, bytes_accessed=6 * heads * q_rows * HD, transcendentals=0),
        name='attn',
    )(q, k, v)


def out_kernel(keep_hbm, send_hbm, wo_hbm, x_hbm, out_hbm, keep_scr, recv_scr, x_scr, w_scr, acc_scr, o_st,
               in_sems, x_sem, w_sems, s_sems, r_sems, o_sems):
    sp = lax.axis_index('sp')
    chip = sp // 2
    core = sp % 2
    partner = chip * 2 + 1 - core
    rows, half = keep_hbm.shape
    bn = w_scr.shape[2]
    tiles = wo_hbm.shape[1] // bn
    slots = w_scr.shape[0]
    pieces = 4
    piece = half // pieces

    def keep_load(i):
        cols = pl.ds(i * piece, piece)
        return pltpu.make_async_copy(keep_hbm.at[:, cols], keep_scr.at[:, cols], in_sems.at[i])

    def exchange(i):
        cols = pl.ds(i * piece, piece)
        return pltpu.make_async_remote_copy(
            src_ref=send_hbm.at[:, cols], dst_ref=recv_scr.at[:, cols], send_sem=s_sems.at[i], recv_sem=r_sems.at[i],
            device_id={'sp': partner}, device_id_type=pl.DeviceIdType.MESH)

    def weight(i):
        side = jnp.where(i < tiles, core, 1 - core)
        r = pl.ds(pl.multiple_of(side * half, half), half)
        c = pl.ds(pl.multiple_of(i % tiles * bn, bn), bn)
        return pltpu.make_async_copy(wo_hbm.at[r, c], w_scr.at[i % slots], w_sems.at[i % slots])

    def first_weight(i):
        r = pl.ds(pl.multiple_of(core * half + i * piece, piece), piece)
        return pltpu.make_async_copy(wo_hbm.at[r, pl.ds(0, bn)], w_scr.at[0, pl.ds(i * piece, piece)], in_sems.at[pieces + i])

    x_load = pltpu.make_async_copy(x_hbm, x_scr, x_sem)

    for i in range(pieces):
        keep_load(i).start()
        first_weight(i).start()
    barrier = pltpu.get_barrier_semaphore()
    pl.semaphore_signal(barrier, inc=1, device_id={'sp': partner}, device_id_type=pl.DeviceIdType.MESH)
    pl.semaphore_wait(barrier, 1)
    for i in range(pieces):
        exchange(i).start()
    for i in range(1, slots - 1):
        weight(i).start()
    x_load.start()

    for i in range(pieces):
        keep_load(i).wait()
        first_weight(i).wait()
        k = slice(i * piece, (i + 1) * piece)
        part = jnp.dot(keep_scr[:, k], w_scr[0, k, :], preferred_element_type=F32)
        acc_scr[0] = part if i == 0 else acc_scr[0] + part
    weight(slots - 1).start()

    def own_half(n, _):
        weight(n).wait()
        weight(n + slots - 1).start()
        acc_scr[n] = jnp.dot(keep_scr[...], w_scr[n % slots], preferred_element_type=F32)
        return 0

    lax.fori_loop(1, tiles, own_half, 0)
    x_load.wait()
    for i in range(pieces):
        exchange(i).wait_recv()

    def store(n, slot):
        return pltpu.make_async_copy(o_st.at[slot], out_hbm.at[:, pl.ds(pl.multiple_of(n * bn, bn), bn)], o_sems.at[slot])

    def other_half(n, _):
        i = n + tiles
        weight(i).wait()

        @pl.when(i + slots - 1 < 2 * tiles)
        def _():
            weight(i + slots - 1).start()

        slot = n % 2

        @pl.when(n >= 2)
        def _():
            store(n - 2, slot).wait()

        cols = pl.ds(pl.multiple_of(n * bn, bn), bn)
        for lo in range(0, rows, rows // 2):
            r = slice(lo, lo + rows // 2)
            total = acc_scr[n, r, :] + jnp.dot(recv_scr[r, :], w_scr[i % slots], preferred_element_type=F32)
            o_st[slot, r, :] = (total + x_scr[r, cols].astype(F32)).astype(BF16)
        store(n, slot).start()
        return 0

    lax.fori_loop(0, tiles, other_half, 0)
    for n in range(tiles - 2, tiles):
        store(n, n % 2).wait()
    for i in range(pieces):
        exchange(i).wait_send()


def out_project(keep, send, w_o, x):
    rows, half = keep.shape
    dim = w_o.shape[1]
    bn = 512
    slots = 4
    dma = pltpu.SemaphoreType.DMA
    return pl.pallas_call(
        out_kernel,
        in_specs=[ANY, ANY, ANY, ANY],
        out_specs=ANY,
        scratch_shapes=[
            pltpu.VMEM((rows, half), BF16),
            pltpu.VMEM((rows, half), BF16),
            pltpu.VMEM((rows, dim), BF16),
            pltpu.VMEM((slots, half, bn), BF16),
            pltpu.VMEM((dim // bn, rows, bn), F32),
            pltpu.VMEM((2, rows, bn), BF16),
            dma((8,)), dma, dma((slots,)), dma((4,)), dma((4,)), dma((2,)),
        ],
        out_shape=jax.ShapeDtypeStruct((rows, dim), BF16),
        compiler_params=pltpu.CompilerParams(vmem_limit_bytes=VMEM_LIMIT, collective_id=1, has_side_effects=True),
        cost_estimate=pl.CostEstimate(flops=4 * rows * half * dim, bytes_accessed=4 * half * dim, transcendentals=0),
        name='out_proj',
    )(keep, send, w_o, x)


def solution(mesh):
    def device_step(hidden, ln_gain, w_q, w_k, w_v, w_o, q_gain, k_gain):
        q, k, v = front(hidden, ln_gain, w_q, w_k, w_v, q_gain, k_gain)
        keep, send = attention(q, k, v)
        return out_project(keep, send, w_o, hidden)

    row_spec = P(('dp', 'sp'), None)
    return jax.shard_map(device_step, mesh=mesh, in_specs=(row_spec, P(), P(), P(), P(), P(), P(), P()), out_specs=row_spec, check_vma=False)
```

```python
import functools
import math

import jax
import jax.numpy as jnp
import numpy as np
from jax import lax
from jax.experimental import pallas as pl
from jax.experimental.pallas import tpu as pltpu
from jax.sharding import PartitionSpec as P

EPS = 1e-6
THETA = 1000000.0
HD = 128
VMEM_LIMIT = 60 * 1024 * 1024
NT = (((1,), (1,)), ((), ()))
F32 = jnp.float32
BF16 = jnp.bfloat16
ANY = pl.BlockSpec(memory_space=pl.ANY)


STRIDE = 64


def rope_parts(seq):
    half = HD // 2
    inv_freq = THETA ** -(np.arange(half) * (2.0 / HD))
    parts = []
    for positions in (np.arange(0, seq, STRIDE), np.arange(STRIDE)):
        angles = positions[:, None] * inv_freq[None, :]
        parts.append(np.concatenate([np.cos(angles), np.cos(angles)], axis=1))
        parts.append(np.concatenate([-np.sin(angles), np.sin(angles)], axis=1))
    return np.concatenate(parts, axis=0).astype(np.float32)


def front_kernel(x_hbm, gain_ref, wq_hbm, wk_hbm, wv_hbm, tab_ref, qgain_ref, kgain_ref, q_out, k_out, v_out,
                 g_ref, qg_ref, kg_ref, cos_ref, sin_ref, own_scr, part_scr, w_scr, ka_scr, va_scr, qa_scr, kv_st, q_st,
                 x_sems, w_sems, xs_sems, xr_sems, loc_sems, ps_sems, pr_sems, cs_sems, cr_sems, q_sems):
    sp = lax.axis_index('sp')
    chip = sp // 2
    core = sp % 2
    partner = chip * 2 + 1 - core
    rows, dim = x_hbm.shape
    bn = w_scr.shape[2]
    part_rows = rows // 4
    q_tiles = wq_hbm.shape[1] // 2 // bn

    def weight(src, col, slot):
        return pltpu.make_async_copy(src.at[:, pl.ds(pl.multiple_of(col, bn), bn)], w_scr.at[slot], w_sems.at[slot])

    def k_weight(s, slot):
        return weight(wk_hbm, (2 * core + s) % 4 * bn, slot)

    def v_weight(s, slot):
        return weight(wv_hbm, (2 * core + s) % 4 * bn, slot)

    def q_weight(n):
        return weight(wq_hbm, core * q_tiles * bn + n * bn, n % 4)

    def x_load(i):
        r = pl.ds(i * part_rows, part_rows)
        return pltpu.make_async_copy(x_hbm.at[r], own_scr.at[r], x_sems.at[i])

    def x_send(i):
        r = pl.ds(pl.multiple_of(i * part_rows, part_rows), part_rows)
        return pltpu.make_async_remote_copy(
            src_ref=x_hbm.at[r], dst_ref=part_scr.at[r], send_sem=xs_sems.at[i], recv_sem=xr_sems.at[i],
            device_id={'sp': partner}, device_id_type=pl.DeviceIdType.MESH)

    def norm(ref, i):
        width = 512
        for sub in range(part_rows // 16):
            r = pl.ds(pl.multiple_of(i * part_rows + sub * 16, 16), 16)
            total = None
            for lo in range(0, dim, width):
                x = ref[r, lo:lo + width].astype(F32)
                x = x * x
                for j in range(0, width, HD):
                    total = x[:, j:j + HD] if total is None else total + x[:, j:j + HD]
            inv = lax.rsqrt(jnp.sum(total, axis=1, keepdims=True) * (1.0 / dim) + EPS)
            for lo in range(0, dim, width):
                x = ref[r, lo:lo + width].astype(F32)
                ref[r, lo:lo + width] = (x * inv * g_ref[:, lo:lo + width]).astype(BF16)

    def rope(acc, at, gain):
        var = jnp.mean(acc * acc, axis=-1, keepdims=True)
        t = acc * lax.rsqrt(var + EPS) * gain[...]
        return t * cos_ref[at, :] + pltpu.roll(t, HD // 2, 1) * sin_ref[at, :]

    def kv_multiply(slot, lo, n):
        r = slice(lo, lo + n)
        ka_scr[r, :] = jnp.dot(own_scr[r, :], w_scr[slot], preferred_element_type=F32)
        va_scr[r, :] = jnp.dot(own_scr[r, :], w_scr[slot + 1], preferred_element_type=F32)

    def kv_put(s):
        for lo in range(0, rows, 128):
            r = slice(lo, lo + 128)
            for i in range(2):
                cols = slice(i * HD, (i + 1) * HD)
                kv_st[s, 0, i, r, :] = rope(ka_scr[r, cols], r, kg_ref).astype(BF16)
                kv_st[s, 1, i, r, :] = va_scr[r, cols].astype(BF16)

    def q_multiply(slot, lo, src):
        qa_scr[lo:lo + rows, :] = jnp.dot(src[...], w_scr[slot], preferred_element_type=F32)

    def q_put(slot, first):
        for lo in range(first, first + rows, 128):
            r = slice(lo, lo + 128)
            for i in range(bn // HD):
                t = rope(qa_scr[r, i * HD:(i + 1) * HD], r, qg_ref)
                length = jnp.sqrt(jnp.sum(t * t, axis=-1, keepdims=True))
                lane = lax.broadcasted_iota(jnp.int32, t.shape, 1)
                q_st[slot, i, r, :HD] = t.astype(BF16)
                q_st[slot, i, r, HD:] = jnp.where(lane == 0, length, 0.0).astype(BF16)

    def q_store(n, slot):
        return pltpu.make_async_copy(q_st.at[slot], q_out.at[pl.ds(n * (bn // HD), bn // HD)], q_sems.at[slot])

    my_rows = pl.ds(pl.multiple_of(chip * 2 * rows + core * rows, rows), rows)
    outs = (k_out, v_out)

    def local(s, i):
        return pltpu.make_async_copy(kv_st.at[s, i], outs[i].at[pl.ds(2 * s, 2), my_rows], loc_sems.at[s, i])

    def to_partner(s, i):
        return pltpu.make_async_remote_copy(
            src_ref=kv_st.at[s, i], dst_ref=outs[i].at[pl.ds(2 * (s - 2), 2), my_rows],
            send_sem=ps_sems.at[s - 2, i], recv_sem=pr_sems.at[s - 2, i],
            device_id={'sp': partner}, device_id_type=pl.DeviceIdType.MESH)

    def across(s, i):
        other = 2 + jnp.where(s < 2, core, 1 - core)
        return pltpu.make_async_remote_copy(
            src_ref=kv_st.at[s, i], dst_ref=outs[i].at[pl.ds(2 * (s % 2), 2), my_rows],
            send_sem=cs_sems.at[s, i], recv_sem=cr_sems.at[core, s % 2, i],
            device_id={'sp': other}, device_id_type=pl.DeviceIdType.MESH)

    def from_across(a, pair, i):
        r = pl.ds(a * rows, rows)
        return pltpu.make_async_remote_copy(
            src_ref=kv_st.at[0, i], dst_ref=outs[i].at[pl.ds(2 * pair, 2), r],
            send_sem=cs_sems.at[0, i], recv_sem=cr_sems.at[a, pair, i],
            device_id={'sp': a}, device_id_type=pl.DeviceIdType.MESH)

    def kv_ship(s):
        for i in range(2):
            @pl.when(s < 2)
            def _():
                local(s, i).start()

            @pl.when(s >= 2)
            def _():
                to_partner(s, i).start()

        @pl.when(chip == 0)
        def _():
            for i in range(2):
                across(s, i).start()

    for i in range(4):
        x_load(i).start()
    k_weight(0, 0).start()
    v_weight(0, 1).start()
    barrier = pltpu.get_barrier_semaphore()
    for d in range(1, 4):
        pl.semaphore_signal(barrier, inc=1, device_id={'sp': (sp + d) % 4}, device_id_type=pl.DeviceIdType.MESH)
    pl.semaphore_wait(barrier, 3)
    for i in range(4):
        x_send(i).start()
    k_weight(1, 2).start()
    v_weight(1, 3).start()

    g_ref[...] = gain_ref[...].astype(F32).reshape(1, dim)
    qg_ref[...] = qgain_ref[...].astype(F32).reshape(1, HD)
    kg_ref[...] = kgain_ref[...].astype(F32).reshape(1, HD)
    coarse = 4 * rows // STRIDE
    cos_b = tab_ref[2 * coarse:2 * coarse + STRIDE, :]
    sin_b = tab_ref[2 * coarse + STRIDE:, :]
    for j in range(2 * rows // STRIDE):
        side = core if j * STRIDE < rows else 1 - core
        a = (chip * 2 + side) * (rows // STRIDE) + j % (rows // STRIDE)
        cos_a = tab_ref[pl.ds(a, 1), :]
        sin_a = tab_ref[pl.ds(coarse + a, 1), :]
        r = slice(j * STRIDE, (j + 1) * STRIDE)
        cos_ref[r, :] = cos_a * cos_b - sin_a * sin_b
        sin_ref[r, :] = sin_a * cos_b + cos_a * sin_b

    for i in range(4):
        x_load(i).wait()

    def norm_own(i, _):
        norm(own_scr, i)
        return 0

    lax.fori_loop(0, 2, norm_own, 0)
    k_weight(0, 0).wait()
    v_weight(0, 1).wait()
    norm(own_scr, 2)
    norm(own_scr, 3)
    kv_multiply(0, 0, rows // 2)
    kv_multiply(0, rows // 2, rows // 2)

    def kv_step(s, _):
        slot = 2 * (s % 2)
        k_weight(s, slot).wait()
        v_weight(s, slot + 1).wait()

        @pl.when(s < 3)
        def _():
            k_weight(s + 1, 2 - slot).start()
            v_weight(s + 1, 3 - slot).start()

        @pl.when(s == 3)
        def _():
            q_weight(0).start()
            q_weight(1).start()

        x_send(s - 1).wait_recv()
        kv_put(s - 1)
        norm(part_scr, s - 1)
        kv_multiply(slot, 0, rows)
        kv_ship(s - 1)
        return 0

    lax.fori_loop(1, 4, kv_step, 0)

    q_weight(0).wait()
    q_weight(2).start()
    q_weight(3).start()
    x_send(3).wait_recv()
    kv_put(3)
    norm(part_scr, 3)
    q_multiply(0, 0, own_scr)
    q_multiply(0, rows, part_scr)
    kv_ship(3)

    def q_step(n, _):
        q_weight(n).wait()

        @pl.when(n + 3 < q_tiles)
        def _():
            q_weight(n + 3).start()

        slot = (n + 1) % 2

        @pl.when(n >= 3)
        def _():
            q_store(n - 3, slot).wait()

        q_put(slot, 0)
        q_multiply(n % 4, 0, own_scr)
        q_put(slot, rows)
        q_multiply(n % 4, rows, part_scr)
        q_store(n - 1, slot).start()
        return 0

    lax.fori_loop(1, q_tiles, q_step, 0)
    slot = (q_tiles - 1) % 2
    q_store(q_tiles - 3, slot).wait()
    q_put(slot, 0)
    q_put(slot, rows)
    q_store(q_tiles - 1, slot).start()

    for i in range(4):
        x_send(i).wait_send()
    for s in range(2):
        for i in range(2):
            local(s, i).wait()
            to_partner(s + 2, i).wait()

    @pl.when(chip == 0)
    def _():
        for s in range(4):
            for i in range(2):
                across(s, i).wait_send()

    @pl.when(chip == 1)
    def _():
        for a in range(2):
            for pair in range(2):
                for i in range(2):
                    from_across(a, pair, i).wait_recv()

    q_store(q_tiles - 2, 1 - slot).wait()
    q_store(q_tiles - 1, slot).wait()


def front(x, gain, w_q, w_k, w_v, q_gain, k_gain):
    rows, dim = x.shape
    bn = 256
    heads = w_q.shape[1] // HD // 2
    kv_heads = w_k.shape[1] // HD // 2
    vmem = pl.BlockSpec(memory_space=pltpu.VMEM)
    kv = jax.ShapeDtypeStruct((kv_heads, 4 * rows, HD), BF16)
    dma = pltpu.SemaphoreType.DMA
    return pl.pallas_call(
        front_kernel,
        in_specs=[ANY, vmem, ANY, ANY, ANY, vmem, vmem, vmem],
        out_specs=[ANY, ANY, ANY],
        out_shape=[jax.ShapeDtypeStruct((heads, 2 * rows, 2 * HD), BF16), kv, kv],
        scratch_shapes=[
            pltpu.VMEM((1, dim), F32),
            pltpu.VMEM((1, HD), F32),
            pltpu.VMEM((1, HD), F32),
            pltpu.VMEM((2 * rows, HD), F32),
            pltpu.VMEM((2 * rows, HD), F32),
            pltpu.VMEM((rows, dim), BF16),
            pltpu.VMEM((rows, dim), BF16),
            pltpu.VMEM((4, dim, bn), BF16),
            pltpu.VMEM((rows, bn), F32),
            pltpu.VMEM((rows, bn), F32),
            pltpu.VMEM((2 * rows, bn), F32),
            pltpu.VMEM((4, 2, 2, rows, HD), BF16),
            pltpu.VMEM((2, bn // HD, 2 * rows, 2 * HD), BF16),
            dma((4,)), dma((4,)), dma((4,)), dma((4,)), dma((2, 2)), dma((2, 2)), dma((2, 2)), dma((4, 2)), dma((2, 2, 2)), dma((2,)),
        ],
        compiler_params=pltpu.CompilerParams(vmem_limit_bytes=VMEM_LIMIT, collective_id=0, has_side_effects=True),
        cost_estimate=pl.CostEstimate(flops=2 * rows * dim * (w_q.shape[1] + 2 * w_k.shape[1]), bytes_accessed=dim * w_q.shape[1], transcendentals=0),
        name='front',
    )(x, gain, w_q, w_k, w_v, jnp.asarray(rope_parts(4 * rows)), q_gain, k_gain)


TILE = 128
KB = 512
SMALL = 2.0 ** -90


def attn_kernel(q_hbm, k_hbm, v_hbm, keep_ref, send_ref, q_scr, k_scr, v_scr, o_scr, low_scr, s_scr, m_scr, q_sems, k_sems, v_sems, o_sems):
    sp = lax.axis_index('sp')
    chip = sp // 2
    core = sp % 2
    groups, seq, _ = k_hbm.shape
    rows = seq // 4
    group = q_scr.shape[0] // groups
    tiles = 2 * rows // TILE
    per = rows // TILE
    scale = HD ** -0.5 * math.log2(math.e)

    def base(tile):
        return (chip * 2 + jnp.where(tile < per, core, 1 - core)) * rows + tile % per * TILE

    def kv_load(g, x):
        span = pl.ds(0, 2 * (x + 1) * rows)
        return [
            pltpu.make_async_copy(src.at[g, span], dst.at[g, span, pl.ds(0, HD)], sems.at[g])
            for src, dst, sems in ((k_hbm, k_scr, k_sems), (v_hbm, v_scr, v_sems))
        ]

    def q_load(t):
        r = pl.ds(t * TILE, TILE)
        return pltpu.make_async_copy(q_hbm.at[:, r], q_scr.at[:, r], q_sems.at[t])

    def kv_start(g):
        for x in range(2):
            @pl.when(chip == x)
            def _():
                for cp in kv_load(g, x):
                    cp.start()

    def kv_wait(g):
        for x in range(2):
            @pl.when(chip == x)
            def _():
                for cp in kv_load(g, x):
                    cp.wait()

    kv_start(0)
    q_load(0).start()
    for g in range(1, groups):
        kv_start(g)
    for t in range(1, tiles):
        q_load(t).start()

    @pl.when(chip == 0)
    def _():
        k_scr[:, 2 * rows:, :HD] = jnp.zeros((groups, 2 * rows, HD), BF16)

    v_scr[:, :, HD:] = jnp.ones((groups, seq, HD), BF16)

    def open_group(g):
        kv_wait(g)
        k = k_scr[g, :, :HD]
        sums = jnp.dot(k * k, jnp.ones((HD, HD), BF16), preferred_element_type=F32)
        longest = jnp.sqrt(jnp.max(sums)) * 1.02
        lane = lax.broadcasted_iota(jnp.int32, (seq, HD), 1)
        k_scr[g, :, HD:] = jnp.where(lane == 0, -longest, 0.0).astype(BF16)
        low_scr[g] = jnp.ones((8, HD), F32)

    def out_copy(ref, slot, tile, g):
        rows_at = pl.ds(pl.multiple_of((tile % per) * TILE, TILE), TILE)
        cols_at = pl.ds(pl.multiple_of(g * group * HD, group * HD), group * HD)
        return pltpu.make_async_copy(o_scr.at[slot], ref.at[rows_at, cols_at], o_sems.at[slot])

    def send_out(slot, tile, g):
        @pl.when(tile < per)
        def _():
            out_copy(keep_ref, slot, tile, g).start()

        @pl.when(tile >= per)
        def _():
            out_copy(send_ref, slot, tile, g).start()

    parts = 2
    hc = group // parts
    mc = hc * TILE

    def run(g, t, slot, off, blocks, width_last):
        total = blocks * KB + width_last
        at = pl.ds(pl.multiple_of(t * TILE, TILE), TILE)
        for c in range(parts):
            q = q_scr[pl.ds(g * group + c * hc, hc), at, :].reshape(mc, 2 * HD)
            ps = []
            for j in range(blocks + 1):
                width = KB if j < blocks else width_last
                s = lax.dot_general(q, k_scr[g, j * KB:j * KB + width, :], NT, preferred_element_type=F32)
                p = jnp.exp2(s * scale)
                if j == blocks:
                    row = lax.broadcasted_iota(jnp.int32, (hc, TILE, width), 1).reshape(mc, width) + off
                    col = lax.broadcasted_iota(jnp.int32, (mc, width), 1)
                    p = jnp.where(row >= col, p, 0.0)
                ps.append(p.astype(BF16))
            p = jnp.concatenate(ps, axis=1) if len(ps) > 1 else ps[0]
            acc = jnp.dot(p, v_scr[g, :total, :], preferred_element_type=F32)
            den = acc[:, HD:]
            o = (acc[:, :HD] * pltpu.reciprocal(den)).astype(BF16)
            for i in range(hc):
                h = c * hc + i
                o_scr[slot, :, h * HD:(h + 1) * HD] = o[i * TILE:(i + 1) * TILE]
            low_scr[g] = jnp.minimum(low_scr[g], jnp.min(den.reshape(mc // 8, 8, HD), axis=0))

    def redo(g, slot):
        def one(step, _):
            tile = step // group
            head = step % group
            q = q_scr[g * group + head, pl.ds(pl.multiple_of(tile * TILE, TILE), TILE), :HD]
            pos = base(tile)
            last = pos // TILE
            row = lax.broadcasted_iota(jnp.int32, (TILE, TILE), 0)
            col = lax.broadcasted_iota(jnp.int32, (TILE, TILE), 1)
            m_scr[...] = jnp.full_like(m_scr, -jnp.inf)

            def first(j, _):
                k = k_scr[g, pl.ds(pl.multiple_of(j * TILE, TILE), TILE), :HD]
                s = lax.dot_general(q, k, NT, preferred_element_type=F32)
                s = jnp.where(row + pos >= col + j * TILE, s, -jnp.inf)
                s_scr[j] = s
                m_scr[...] = jnp.maximum(m_scr[...], s)
                return 0

            lax.fori_loop(0, last + 1, first, 0)
            m = jnp.max(m_scr[...], axis=1, keepdims=True)

            def second(j, acc):
                p = jnp.exp2((s_scr[j] - m) * scale).astype(BF16)
                v = v_scr[g, pl.ds(pl.multiple_of(j * TILE, TILE), TILE), :]
                return acc + jnp.dot(p, v, preferred_element_type=F32)

            acc = lax.fori_loop(0, last + 1, second, jnp.zeros((TILE, 2 * HD), F32))
            o = (acc[:, :HD] / acc[:, HD:]).astype(BF16)
            for h in range(group):
                @pl.when(head == h)
                def _():
                    o_scr[slot, :, h * HD:(h + 1) * HD] = o

            @pl.when(head == group - 1)
            def _():
                send_out(slot, tile, g)
                out_copy(keep_ref, slot, 0, 0).wait()

            return 0

        lax.fori_loop(0, tiles * group, one, 0)

    def step(it, _):
        t = it // groups
        g = it % groups
        slot = it % 2

        @pl.when(g == 0)
        def _():
            q_load(t).wait()

        @pl.when(t == 0)
        def _():
            open_group(g)

        @pl.when(it >= 2)
        def _():
            out_copy(keep_ref, slot, 0, 0).wait()

        pos0 = base(t)
        nfull = pos0 // KB
        off = pos0 - nfull * KB
        for upper in range(2):
            @pl.when(nfull // 2 == upper)
            def _():
                for low in range(2):
                    @pl.when(nfull % 2 == low)
                    def _():
                        for half in range(2):
                            @pl.when(off // 256 == half)
                            def _():
                                run(g, t, slot, off, 2 * upper + low, (half + 1) * 256)

        send_out(slot, t, g)
        return 0

    lax.fori_loop(0, groups * tiles, step, 0)
    for slot in range(2):
        out_copy(keep_ref, slot, 0, 0).wait()

    @pl.when(jnp.min(low_scr[...]) < SMALL)
    def _():
        def group_again(g, _):
            redo(g, 0)
            return 0

        lax.fori_loop(0, groups, group_again, 0)


def attention(q, k, v):
    heads, q_rows, _ = q.shape
    groups, seq, _ = k.shape
    group = heads // groups
    out = jax.ShapeDtypeStruct((q_rows // 2, heads * HD), BF16)
    dma = pltpu.SemaphoreType.DMA
    return pl.pallas_call(
        attn_kernel,
        in_specs=[ANY, ANY, ANY],
        out_specs=[ANY, ANY],
        scratch_shapes=[
            pltpu.VMEM((heads, q_rows, 2 * HD), BF16),
            pltpu.VMEM((groups, seq, 2 * HD), BF16),
            pltpu.VMEM((groups, seq, 2 * HD), BF16),
            pltpu.VMEM((2, TILE, group * HD), BF16),
            pltpu.VMEM((groups, 8, HD), F32),
            pltpu.VMEM((seq // TILE, TILE, TILE), F32),
            pltpu.VMEM((TILE, TILE), F32),
            dma((q_rows // TILE,)), dma((groups,)), dma((groups,)), dma((2,)),
        ],
        out_shape=[out, out],
        compiler_params=pltpu.CompilerParams(vmem_limit_bytes=VMEM_LIMIT),
        cost_estimate=pl.CostEstimate(flops=4 * heads * q_rows * seq * HD, bytes_accessed=6 * heads * q_rows * HD, transcendentals=0),
        name='attn',
    )(q, k, v)


def out_kernel(keep_hbm, send_hbm, wo_hbm, x_hbm, out_hbm, keep_scr, recv_scr, x_scr, w_scr, acc_scr, o_st,
               in_sems, x_sem, w_sems, s_sems, r_sems, o_sems):
    sp = lax.axis_index('sp')
    chip = sp // 2
    core = sp % 2
    partner = chip * 2 + 1 - core
    rows, half = keep_hbm.shape
    bn = w_scr.shape[2]
    tiles = wo_hbm.shape[1] // bn
    slots = w_scr.shape[0]
    pieces = 4
    piece = half // pieces

    def keep_load(i):
        cols = pl.ds(i * piece, piece)
        return pltpu.make_async_copy(keep_hbm.at[:, cols], keep_scr.at[:, cols], in_sems.at[i])

    def exchange(i):
        cols = pl.ds(i * piece, piece)
        return pltpu.make_async_remote_copy(
            src_ref=send_hbm.at[:, cols], dst_ref=recv_scr.at[:, cols], send_sem=s_sems.at[i], recv_sem=r_sems.at[i],
            device_id={'sp': partner}, device_id_type=pl.DeviceIdType.MESH)

    def weight(i):
        side = jnp.where(i < tiles, core, 1 - core)
        r = pl.ds(pl.multiple_of(side * half, half), half)
        c = pl.ds(pl.multiple_of(i % tiles * bn, bn), bn)
        return pltpu.make_async_copy(wo_hbm.at[r, c], w_scr.at[i % slots], w_sems.at[i % slots])

    def first_weight(i):
        r = pl.ds(pl.multiple_of(core * half + i * piece, piece), piece)
        return pltpu.make_async_copy(wo_hbm.at[r, pl.ds(0, bn)], w_scr.at[0, pl.ds(i * piece, piece)], in_sems.at[pieces + i])

    x_load = pltpu.make_async_copy(x_hbm, x_scr, x_sem)

    for i in range(pieces):
        keep_load(i).start()
        first_weight(i).start()
    barrier = pltpu.get_barrier_semaphore()
    pl.semaphore_signal(barrier, inc=1, device_id={'sp': partner}, device_id_type=pl.DeviceIdType.MESH)
    pl.semaphore_wait(barrier, 1)
    for i in range(pieces):
        exchange(i).start()
    for i in range(1, slots - 1):
        weight(i).start()
    x_load.start()

    for i in range(pieces):
        keep_load(i).wait()
        first_weight(i).wait()
        k = slice(i * piece, (i + 1) * piece)
        part = jnp.dot(keep_scr[:, k], w_scr[0, k, :], preferred_element_type=F32)
        acc_scr[0] = part if i == 0 else acc_scr[0] + part
    weight(slots - 1).start()

    def own_half(n, _):
        weight(n).wait()
        weight(n + slots - 1).start()
        acc_scr[n] = jnp.dot(keep_scr[...], w_scr[n % slots], preferred_element_type=F32)
        return 0

    lax.fori_loop(1, tiles, own_half, 0)
    x_load.wait()
    for i in range(pieces):
        exchange(i).wait_recv()

    def store(n, slot):
        return pltpu.make_async_copy(o_st.at[slot], out_hbm.at[:, pl.ds(pl.multiple_of(n * bn, bn), bn)], o_sems.at[slot])

    def other_half(n, _):
        i = n + tiles
        weight(i).wait()

        @pl.when(i + slots - 1 < 2 * tiles)
        def _():
            weight(i + slots - 1).start()

        slot = n % 2

        @pl.when(n >= 2)
        def _():
            store(n - 2, slot).wait()

        cols = pl.ds(pl.multiple_of(n * bn, bn), bn)
        for lo in range(0, rows, rows // 2):
            r = slice(lo, lo + rows // 2)
            total = acc_scr[n, r, :] + jnp.dot(recv_scr[r, :], w_scr[i % slots], preferred_element_type=F32)
            o_st[slot, r, :] = (total + x_scr[r, cols].astype(F32)).astype(BF16)
        store(n, slot).start()
        return 0

    lax.fori_loop(0, tiles, other_half, 0)
    for n in range(tiles - 2, tiles):
        store(n, n % 2).wait()
    for i in range(pieces):
        exchange(i).wait_send()


def out_project(keep, send, w_o, x):
    rows, half = keep.shape
    dim = w_o.shape[1]
    bn = 512
    slots = 4
    dma = pltpu.SemaphoreType.DMA
    return pl.pallas_call(
        out_kernel,
        in_specs=[ANY, ANY, ANY, ANY],
        out_specs=ANY,
        scratch_shapes=[
            pltpu.VMEM((rows, half), BF16),
            pltpu.VMEM((rows, half), BF16),
            pltpu.VMEM((rows, dim), BF16),
            pltpu.VMEM((slots, half, bn), BF16),
            pltpu.VMEM((dim // bn, rows, bn), F32),
            pltpu.VMEM((2, rows, bn), BF16),
            dma((8,)), dma, dma((slots,)), dma((4,)), dma((4,)), dma((2,)),
        ],
        out_shape=jax.ShapeDtypeStruct((rows, dim), BF16),
        compiler_params=pltpu.CompilerParams(vmem_limit_bytes=VMEM_LIMIT, collective_id=1, has_side_effects=True),
        cost_estimate=pl.CostEstimate(flops=4 * rows * half * dim, bytes_accessed=4 * half * dim, transcendentals=0),
        name='out_proj',
    )(keep, send, w_o, x)


def solution(mesh):
    def device_step(hidden, ln_gain, w_q, w_k, w_v, w_o, q_gain, k_gain):
        q, k, v = front(hidden, ln_gain, w_q, w_k, w_v, q_gain, k_gain)
        keep, send = attention(q, k, v)
        return out_project(keep, send, w_o, hidden)

    row_spec = P(('dp', 'sp'), None)
    return jax.shard_map(device_step, mesh=mesh, in_specs=(row_spec, P(), P(), P(), P(), P(), P(), P()), out_specs=row_spec, check_vma=False)
```

```python
import functools
import math

import jax
import jax.numpy as jnp
import numpy as np
from jax import lax
from jax.experimental import pallas as pl
from jax.experimental.pallas import tpu as pltpu
from jax.sharding import PartitionSpec as P

EPS = 1e-6
THETA = 1000000.0
HD = 128
VMEM_LIMIT = 60 * 1024 * 1024
NT = (((1,), (1,)), ((), ()))
F32 = jnp.float32
BF16 = jnp.bfloat16
ANY = pl.BlockSpec(memory_space=pl.ANY)


STRIDE = 64


def rope_parts(seq):
    half = HD // 2
    inv_freq = THETA ** -(np.arange(half) * (2.0 / HD))
    parts = []
    for positions in (np.arange(0, seq, STRIDE), np.arange(STRIDE)):
        angles = positions[:, None] * inv_freq[None, :]
        parts.append(np.concatenate([np.cos(angles), np.cos(angles)], axis=1))
        parts.append(np.concatenate([-np.sin(angles), np.sin(angles)], axis=1))
    return np.concatenate(parts, axis=0).astype(np.float32)


def front_kernel(x_hbm, gain_ref, wq_hbm, wk_hbm, wv_hbm, tab_ref, qgain_ref, kgain_ref, q_out, k_out, v_out,
                 g_ref, qg_ref, kg_ref, cos_ref, sin_ref, own_scr, part_scr, w_scr, ka_scr, va_scr, qa_scr, kv_st, q_st,
                 x_sems, w_sems, xs_sems, xr_sems, loc_sems, ps_sems, pr_sems, cs_sems, cr_sems, q_sems):
    sp = lax.axis_index('sp')
    chip = sp // 2
    core = sp % 2
    partner = chip * 2 + 1 - core
    rows, dim = x_hbm.shape
    bn = w_scr.shape[2]
    part_rows = rows // 4
    q_tiles = wq_hbm.shape[1] // 2 // bn

    def weight(src, col, slot):
        return pltpu.make_async_copy(src.at[:, pl.ds(pl.multiple_of(col, bn), bn)], w_scr.at[slot], w_sems.at[slot])

    def k_weight(s, slot):
        return weight(wk_hbm, (2 * core + s) % 4 * bn, slot)

    def v_weight(s, slot):
        return weight(wv_hbm, (2 * core + s) % 4 * bn, slot)

    def q_weight(n):
        return weight(wq_hbm, core * q_tiles * bn + n * bn, n % 4)

    def x_load(i):
        r = pl.ds(pl.multiple_of(i * part_rows, part_rows), part_rows)
        return pltpu.make_async_copy(x_hbm.at[r], own_scr.at[r], x_sems.at[i])

    def x_send(i):
        r = pl.ds(pl.multiple_of(i * part_rows, part_rows), part_rows)
        return pltpu.make_async_remote_copy(
            src_ref=x_hbm.at[r], dst_ref=part_scr.at[r], send_sem=xs_sems.at[i], recv_sem=xr_sems.at[i],
            device_id={'sp': partner}, device_id_type=pl.DeviceIdType.MESH)

    def norm(ref, i):
        width = 512
        for sub in range(part_rows // 16):
            r = pl.ds(pl.multiple_of(i * part_rows + sub * 16, 16), 16)
            total = None
            for lo in range(0, dim, width):
                x = ref[r, lo:lo + width].astype(F32)
                x = x * x
                for j in range(0, width, HD):
                    total = x[:, j:j + HD] if total is None else total + x[:, j:j + HD]
            inv = lax.rsqrt(jnp.sum(total, axis=1, keepdims=True) * (1.0 / dim) + EPS)
            for lo in range(0, dim, width):
                x = ref[r, lo:lo + width].astype(F32)
                ref[r, lo:lo + width] = (x * inv * g_ref[:, lo:lo + width]).astype(BF16)

    def rope(acc, at, gain):
        var = jnp.mean(acc * acc, axis=-1, keepdims=True)
        t = acc * lax.rsqrt(var + EPS) * gain[...]
        return t * cos_ref[at, :] + pltpu.roll(t, HD // 2, 1) * sin_ref[at, :]

    def kv_multiply(slot, lo, n):
        r = slice(lo, lo + n)
        ka_scr[r, :] = jnp.dot(own_scr[r, :], w_scr[slot], preferred_element_type=F32)
        va_scr[r, :] = jnp.dot(own_scr[r, :], w_scr[slot + 1], preferred_element_type=F32)

    def kv_put(s):
        for lo in range(0, rows, 128):
            r = slice(lo, lo + 128)
            for i in range(2):
                cols = slice(i * HD, (i + 1) * HD)
                kv_st[s, 0, i, r, :] = rope(ka_scr[r, cols], r, kg_ref).astype(BF16)
                kv_st[s, 1, i, r, :] = va_scr[r, cols].astype(BF16)

    def q_multiply(slot, lo, src):
        qa_scr[lo:lo + rows, :] = jnp.dot(src[...], w_scr[slot], preferred_element_type=F32)

    def q_put(slot, first):
        for lo in range(first, first + rows, 128):
            r = slice(lo, lo + 128)
            for i in range(bn // HD):
                t = rope(qa_scr[r, i * HD:(i + 1) * HD], r, qg_ref)
                length = jnp.sqrt(jnp.sum(t * t, axis=-1, keepdims=True))
                lane = lax.broadcasted_iota(jnp.int32, t.shape, 1)
                q_st[slot, i, r, :HD] = t.astype(BF16)
                q_st[slot, i, r, HD:] = jnp.where(lane == 0, length, 0.0).astype(BF16)

    def q_store(n, slot):
        return pltpu.make_async_copy(q_st.at[slot], q_out.at[pl.ds(n * (bn // HD), bn // HD)], q_sems.at[slot])

    my_rows = pl.ds(pl.multiple_of(chip * 2 * rows + core * rows, rows), rows)
    outs = (k_out, v_out)

    def local(s, i):
        return pltpu.make_async_copy(kv_st.at[s, i], outs[i].at[pl.ds(2 * s, 2), my_rows], loc_sems.at[s, i])

    def to_partner(s, i):
        return pltpu.make_async_remote_copy(
            src_ref=kv_st.at[s, i], dst_ref=outs[i].at[pl.ds(2 * (s - 2), 2), my_rows],
            send_sem=ps_sems.at[s - 2, i], recv_sem=pr_sems.at[s - 2, i],
            device_id={'sp': partner}, device_id_type=pl.DeviceIdType.MESH)

    def across(s, i):
        other = 2 + jnp.where(s < 2, core, 1 - core)
        return pltpu.make_async_remote_copy(
            src_ref=kv_st.at[s, i], dst_ref=outs[i].at[pl.ds(2 * (s % 2), 2), my_rows],
            send_sem=cs_sems.at[s, i], recv_sem=cr_sems.at[core, s % 2, i],
            device_id={'sp': other}, device_id_type=pl.DeviceIdType.MESH)

    def from_across(a, pair, i):
        r = pl.ds(a * rows, rows)
        return pltpu.make_async_remote_copy(
            src_ref=kv_st.at[0, i], dst_ref=outs[i].at[pl.ds(2 * pair, 2), r],
            send_sem=cs_sems.at[0, i], recv_sem=cr_sems.at[a, pair, i],
            device_id={'sp': a}, device_id_type=pl.DeviceIdType.MESH)

    def kv_ship(s):
        for i in range(2):
            @pl.when(s < 2)
            def _():
                local(s, i).start()

            @pl.when(s >= 2)
            def _():
                to_partner(s, i).start()

        @pl.when(chip == 0)
        def _():
            for i in range(2):
                across(s, i).start()

    for i in range(4):
        x_load(i).start()
    k_weight(0, 0).start()
    v_weight(0, 1).start()
    barrier = pltpu.get_barrier_semaphore()
    for d in range(1, 4):
        pl.semaphore_signal(barrier, inc=1, device_id={'sp': (sp + d) % 4}, device_id_type=pl.DeviceIdType.MESH)
    pl.semaphore_wait(barrier, 3)
    for i in range(4):
        x_send(i).start()
    k_weight(1, 2).start()
    v_weight(1, 3).start()

    g_ref[...] = gain_ref[...].astype(F32).reshape(1, dim)
    qg_ref[...] = qgain_ref[...].astype(F32).reshape(1, HD)
    kg_ref[...] = kgain_ref[...].astype(F32).reshape(1, HD)
    coarse = 4 * rows // STRIDE
    cos_b = tab_ref[2 * coarse:2 * coarse + STRIDE, :]
    sin_b = tab_ref[2 * coarse + STRIDE:, :]
    for j in range(2 * rows // STRIDE):
        side = core if j * STRIDE < rows else 1 - core
        a = (chip * 2 + side) * (rows // STRIDE) + j % (rows // STRIDE)
        cos_a = tab_ref[pl.ds(a, 1), :]
        sin_a = tab_ref[pl.ds(coarse + a, 1), :]
        r = slice(j * STRIDE, (j + 1) * STRIDE)
        cos_ref[r, :] = cos_a * cos_b - sin_a * sin_b
        sin_ref[r, :] = sin_a * cos_b + cos_a * sin_b

    def norm_own(i, _):
        x_load(i).wait()
        norm(own_scr, i)
        return 0

    lax.fori_loop(0, 2, norm_own, 0)
    x_load(2).wait()
    x_load(3).wait()
    k_weight(0, 0).wait()
    v_weight(0, 1).wait()
    norm(own_scr, 2)
    norm(own_scr, 3)
    kv_multiply(0, 0, rows // 2)
    kv_multiply(0, rows // 2, rows // 2)

    def kv_step(s, _):
        slot = 2 * (s % 2)
        k_weight(s, slot).wait()
        v_weight(s, slot + 1).wait()

        @pl.when(s < 3)
        def _():
            k_weight(s + 1, 2 - slot).start()
            v_weight(s + 1, 3 - slot).start()

        @pl.when(s == 3)
        def _():
            q_weight(0).start()
            q_weight(1).start()

        x_send(s - 1).wait_recv()
        kv_put(s - 1)
        norm(part_scr, s - 1)
        kv_multiply(slot, 0, rows)
        kv_ship(s - 1)
        return 0

    lax.fori_loop(1, 4, kv_step, 0)

    q_weight(0).wait()
    q_weight(2).start()
    q_weight(3).start()
    x_send(3).wait_recv()
    kv_put(3)
    norm(part_scr, 3)
    q_multiply(0, 0, own_scr)
    q_multiply(0, rows, part_scr)
    kv_ship(3)

    def q_step(n, _):
        q_weight(n).wait()

        @pl.when(n + 3 < q_tiles)
        def _():
            q_weight(n + 3).start()

        slot = (n + 1) % 2

        @pl.when(n >= 3)
        def _():
            q_store(n - 3, slot).wait()

        q_put(slot, 0)
        q_multiply(n % 4, 0, own_scr)
        q_put(slot, rows)
        q_multiply(n % 4, rows, part_scr)
        q_store(n - 1, slot).start()
        return 0

    lax.fori_loop(1, q_tiles, q_step, 0)
    slot = (q_tiles - 1) % 2
    q_store(q_tiles - 3, slot).wait()
    q_put(slot, 0)
    q_put(slot, rows)
    q_store(q_tiles - 1, slot).start()

    for i in range(4):
        x_send(i).wait_send()
    for s in range(2):
        for i in range(2):
            local(s, i).wait()
            to_partner(s + 2, i).wait()

    @pl.when(chip == 0)
    def _():
        for s in range(4):
            for i in range(2):
                across(s, i).wait_send()

    @pl.when(chip == 1)
    def _():
        for a in range(2):
            for pair in range(2):
                for i in range(2):
                    from_across(a, pair, i).wait_recv()

    q_store(q_tiles - 2, 1 - slot).wait()
    q_store(q_tiles - 1, slot).wait()


def front(x, gain, w_q, w_k, w_v, q_gain, k_gain):
    rows, dim = x.shape
    bn = 256
    heads = w_q.shape[1] // HD // 2
    kv_heads = w_k.shape[1] // HD // 2
    vmem = pl.BlockSpec(memory_space=pltpu.VMEM)
    kv = jax.ShapeDtypeStruct((kv_heads, 4 * rows, HD), BF16)
    dma = pltpu.SemaphoreType.DMA
    return pl.pallas_call(
        front_kernel,
        in_specs=[ANY, vmem, ANY, ANY, ANY, vmem, vmem, vmem],
        out_specs=[ANY, ANY, ANY],
        out_shape=[jax.ShapeDtypeStruct((heads, 2 * rows, 2 * HD), BF16), kv, kv],
        scratch_shapes=[
            pltpu.VMEM((1, dim), F32),
            pltpu.VMEM((1, HD), F32),
            pltpu.VMEM((1, HD), F32),
            pltpu.VMEM((2 * rows, HD), F32),
            pltpu.VMEM((2 * rows, HD), F32),
            pltpu.VMEM((rows, dim), BF16),
            pltpu.VMEM((rows, dim), BF16),
            pltpu.VMEM((4, dim, bn), BF16),
            pltpu.VMEM((rows, bn), F32),
            pltpu.VMEM((rows, bn), F32),
            pltpu.VMEM((2 * rows, bn), F32),
            pltpu.VMEM((4, 2, 2, rows, HD), BF16),
            pltpu.VMEM((2, bn // HD, 2 * rows, 2 * HD), BF16),
            dma((4,)), dma((4,)), dma((4,)), dma((4,)), dma((2, 2)), dma((2, 2)), dma((2, 2)), dma((4, 2)), dma((2, 2, 2)), dma((2,)),
        ],
        compiler_params=pltpu.CompilerParams(vmem_limit_bytes=VMEM_LIMIT, collective_id=0, has_side_effects=True),
        cost_estimate=pl.CostEstimate(flops=2 * rows * dim * (w_q.shape[1] + 2 * w_k.shape[1]), bytes_accessed=dim * w_q.shape[1], transcendentals=0),
        name='front',
    )(x, gain, w_q, w_k, w_v, jnp.asarray(rope_parts(4 * rows)), q_gain, k_gain)


TILE = 128
KB = 512
SMALL = 2.0 ** -90


def attn_kernel(q_hbm, k_hbm, v_hbm, keep_ref, send_ref, q_scr, k_scr, v_scr, o_scr, low_scr, s_scr, m_scr, q_sems, k_sems, v_sems, o_sems):
    sp = lax.axis_index('sp')
    chip = sp // 2
    core = sp % 2
    groups, seq, _ = k_hbm.shape
    rows = seq // 4
    group = q_scr.shape[0] // groups
    tiles = 2 * rows // TILE
    per = rows // TILE
    scale = HD ** -0.5 * math.log2(math.e)

    def base(tile):
        return (chip * 2 + jnp.where(tile < per, core, 1 - core)) * rows + tile % per * TILE

    def kv_load(g, x):
        span = pl.ds(0, 2 * (x + 1) * rows)
        return [
            pltpu.make_async_copy(src.at[g, span], dst.at[g, span, pl.ds(0, HD)], sems.at[g])
            for src, dst, sems in ((k_hbm, k_scr, k_sems), (v_hbm, v_scr, v_sems))
        ]

    def q_load(t):
        r = pl.ds(t * TILE, TILE)
        return pltpu.make_async_copy(q_hbm.at[:, r], q_scr.at[:, r], q_sems.at[t])

    def kv_start(g):
        for x in range(2):
            @pl.when(chip == x)
            def _():
                for cp in kv_load(g, x):
                    cp.start()

    def kv_wait(g):
        for x in range(2):
            @pl.when(chip == x)
            def _():
                for cp in kv_load(g, x):
                    cp.wait()

    kv_start(0)
    q_load(0).start()
    for g in range(1, groups):
        kv_start(g)
    for t in range(1, tiles):
        q_load(t).start()

    @pl.when(chip == 0)
    def _():
        k_scr[:, 2 * rows:, :HD] = jnp.zeros((groups, 2 * rows, HD), BF16)

    v_scr[:, :, HD:] = jnp.ones((groups, seq, HD), BF16)

    def open_group(g):
        kv_wait(g)
        k = k_scr[g, :, :HD]
        sums = jnp.dot(k * k, jnp.ones((HD, HD), BF16), preferred_element_type=F32)
        longest = jnp.sqrt(jnp.max(sums)) * 1.02
        lane = lax.broadcasted_iota(jnp.int32, (seq, HD), 1)
        k_scr[g, :, HD:] = jnp.where(lane == 0, -longest, 0.0).astype(BF16)
        low_scr[g] = jnp.ones((8, HD), F32)

    def out_copy(ref, slot, tile, g):
        rows_at = pl.ds(pl.multiple_of((tile % per) * TILE, TILE), TILE)
        cols_at = pl.ds(pl.multiple_of(g * group * HD, group * HD), group * HD)
        return pltpu.make_async_copy(o_scr.at[slot], ref.at[rows_at, cols_at], o_sems.at[slot])

    def send_out(slot, tile, g):
        @pl.when(tile < per)
        def _():
            out_copy(keep_ref, slot, tile, g).start()

        @pl.when(tile >= per)
        def _():
            out_copy(send_ref, slot, tile, g).start()

    parts = 2
    hc = group // parts
    mc = hc * TILE

    def run(g, t, slot, off, blocks, width_last):
        total = blocks * KB + width_last
        at = pl.ds(pl.multiple_of(t * TILE, TILE), TILE)
        for c in range(parts):
            q = q_scr[pl.ds(g * group + c * hc, hc), at, :].reshape(mc, 2 * HD)
            ps = []
            for j in range(blocks + 1):
                width = KB if j < blocks else width_last
                s = lax.dot_general(q, k_scr[g, j * KB:j * KB + width, :], NT, preferred_element_type=F32)
                p = jnp.exp2(s * scale)
                if j == blocks:
                    row = lax.broadcasted_iota(jnp.int32, (hc, TILE, width), 1).reshape(mc, width) + off
                    col = lax.broadcasted_iota(jnp.int32, (mc, width), 1)
                    p = jnp.where(row >= col, p, 0.0)
                ps.append(p.astype(BF16))
            p = jnp.concatenate(ps, axis=1) if len(ps) > 1 else ps[0]
            acc = jnp.dot(p, v_scr[g, :total, :], preferred_element_type=F32)
            den = acc[:, HD:]
            o = (acc[:, :HD] * pltpu.reciprocal(den)).astype(BF16)
            for i in range(hc):
                h = c * hc + i
                o_scr[slot, :, h * HD:(h + 1) * HD] = o[i * TILE:(i + 1) * TILE]
            low_scr[g] = jnp.minimum(low_scr[g], jnp.min(den.reshape(mc // 8, 8, HD), axis=0))

    def redo(g, slot):
        def one(step, _):
            tile = step // group
            head = step % group
            q = q_scr[g * group + head, pl.ds(pl.multiple_of(tile * TILE, TILE), TILE), :HD]
            pos = base(tile)
            last = pos // TILE
            row = lax.broadcasted_iota(jnp.int32, (TILE, TILE), 0)
            col = lax.broadcasted_iota(jnp.int32, (TILE, TILE), 1)
            m_scr[...] = jnp.full_like(m_scr, -jnp.inf)

            def first(j, _):
                k = k_scr[g, pl.ds(pl.multiple_of(j * TILE, TILE), TILE), :HD]
                s = lax.dot_general(q, k, NT, preferred_element_type=F32)
                s = jnp.where(row + pos >= col + j * TILE, s, -jnp.inf)
                s_scr[j] = s
                m_scr[...] = jnp.maximum(m_scr[...], s)
                return 0

            lax.fori_loop(0, last + 1, first, 0)
            m = jnp.max(m_scr[...], axis=1, keepdims=True)

            def second(j, acc):
                p = jnp.exp2((s_scr[j] - m) * scale).astype(BF16)
                v = v_scr[g, pl.ds(pl.multiple_of(j * TILE, TILE), TILE), :]
                return acc + jnp.dot(p, v, preferred_element_type=F32)

            acc = lax.fori_loop(0, last + 1, second, jnp.zeros((TILE, 2 * HD), F32))
            o = (acc[:, :HD] / acc[:, HD:]).astype(BF16)
            for h in range(group):
                @pl.when(head == h)
                def _():
                    o_scr[slot, :, h * HD:(h + 1) * HD] = o

            @pl.when(head == group - 1)
            def _():
                send_out(slot, tile, g)
                out_copy(keep_ref, slot, 0, 0).wait()

            return 0

        lax.fori_loop(0, tiles * group, one, 0)

    def step(it, _):
        t = it // groups
        g = it % groups
        slot = it % 2

        @pl.when(g == 0)
        def _():
            q_load(t).wait()

        @pl.when(t == 0)
        def _():
            open_group(g)

        @pl.when(it >= 2)
        def _():
            out_copy(keep_ref, slot, 0, 0).wait()

        pos0 = base(t)
        nfull = pos0 // KB
        off = pos0 - nfull * KB
        for upper in range(2):
            @pl.when(nfull // 2 == upper)
            def _():
                for low in range(2):
                    @pl.when(nfull % 2 == low)
                    def _():
                        for half in range(2):
                            @pl.when(off // 256 == half)
                            def _():
                                run(g, t, slot, off, 2 * upper + low, (half + 1) * 256)

        send_out(slot, t, g)
        return 0

    lax.fori_loop(0, groups * tiles, step, 0)
    for slot in range(2):
        out_copy(keep_ref, slot, 0, 0).wait()

    @pl.when(jnp.min(low_scr[...]) < SMALL)
    def _():
        def group_again(g, _):
            redo(g, 0)
            return 0

        lax.fori_loop(0, groups, group_again, 0)


def attention(q, k, v):
    heads, q_rows, _ = q.shape
    groups, seq, _ = k.shape
    group = heads // groups
    out = jax.ShapeDtypeStruct((q_rows // 2, heads * HD), BF16)
    dma = pltpu.SemaphoreType.DMA
    return pl.pallas_call(
        attn_kernel,
        in_specs=[ANY, ANY, ANY],
        out_specs=[ANY, ANY],
        scratch_shapes=[
            pltpu.VMEM((heads, q_rows, 2 * HD), BF16),
            pltpu.VMEM((groups, seq, 2 * HD), BF16),
            pltpu.VMEM((groups, seq, 2 * HD), BF16),
            pltpu.VMEM((2, TILE, group * HD), BF16),
            pltpu.VMEM((groups, 8, HD), F32),
            pltpu.VMEM((seq // TILE, TILE, TILE), F32),
            pltpu.VMEM((TILE, TILE), F32),
            dma((q_rows // TILE,)), dma((groups,)), dma((groups,)), dma((2,)),
        ],
        out_shape=[out, out],
        compiler_params=pltpu.CompilerParams(vmem_limit_bytes=VMEM_LIMIT),
        cost_estimate=pl.CostEstimate(flops=4 * heads * q_rows * seq * HD, bytes_accessed=6 * heads * q_rows * HD, transcendentals=0),
        name='attn',
    )(q, k, v)


def out_kernel(keep_hbm, send_hbm, wo_hbm, x_hbm, out_hbm, keep_scr, recv_scr, x_scr, w_scr, acc_scr, o_st,
               in_sems, x_sem, w_sems, s_sems, r_sems, o_sems):
    sp = lax.axis_index('sp')
    chip = sp // 2
    core = sp % 2
    partner = chip * 2 + 1 - core
    rows, half = keep_hbm.shape
    bn = w_scr.shape[2]
    tiles = wo_hbm.shape[1] // bn
    slots = w_scr.shape[0]
    pieces = 4
    piece = half // pieces

    def keep_load(i):
        cols = pl.ds(i * piece, piece)
        return pltpu.make_async_copy(keep_hbm.at[:, cols], keep_scr.at[:, cols], in_sems.at[i])

    def exchange(i):
        cols = pl.ds(i * piece, piece)
        return pltpu.make_async_remote_copy(
            src_ref=send_hbm.at[:, cols], dst_ref=recv_scr.at[:, cols], send_sem=s_sems.at[i], recv_sem=r_sems.at[i],
            device_id={'sp': partner}, device_id_type=pl.DeviceIdType.MESH)

    def weight(i):
        side = jnp.where(i < tiles, core, 1 - core)
        r = pl.ds(pl.multiple_of(side * half, half), half)
        c = pl.ds(pl.multiple_of(i % tiles * bn, bn), bn)
        return pltpu.make_async_copy(wo_hbm.at[r, c], w_scr.at[i % slots], w_sems.at[i % slots])

    def first_weight(i):
        r = pl.ds(pl.multiple_of(core * half + i * piece, piece), piece)
        return pltpu.make_async_copy(wo_hbm.at[r, pl.ds(0, bn)], w_scr.at[0, pl.ds(i * piece, piece)], in_sems.at[pieces + i])

    x_load = pltpu.make_async_copy(x_hbm, x_scr, x_sem)

    for i in range(pieces):
        keep_load(i).start()
        first_weight(i).start()
    barrier = pltpu.get_barrier_semaphore()
    pl.semaphore_signal(barrier, inc=1, device_id={'sp': partner}, device_id_type=pl.DeviceIdType.MESH)
    pl.semaphore_wait(barrier, 1)
    for i in range(pieces):
        exchange(i).start()
    for i in range(1, slots - 1):
        weight(i).start()
    x_load.start()

    for i in range(pieces):
        keep_load(i).wait()
        first_weight(i).wait()
        k = slice(i * piece, (i + 1) * piece)
        part = jnp.dot(keep_scr[:, k], w_scr[0, k, :], preferred_element_type=F32)
        acc_scr[0] = part if i == 0 else acc_scr[0] + part
    weight(slots - 1).start()

    def own_half(n, _):
        weight(n).wait()
        weight(n + slots - 1).start()
        acc_scr[n] = jnp.dot(keep_scr[...], w_scr[n % slots], preferred_element_type=F32)
        return 0

    lax.fori_loop(1, tiles, own_half, 0)
    x_load.wait()
    for i in range(pieces):
        exchange(i).wait_recv()

    def store(n, slot):
        return pltpu.make_async_copy(o_st.at[slot], out_hbm.at[:, pl.ds(pl.multiple_of(n * bn, bn), bn)], o_sems.at[slot])

    def other_half(n, _):
        i = n + tiles
        weight(i).wait()

        @pl.when(i + slots - 1 < 2 * tiles)
        def _():
            weight(i + slots - 1).start()

        slot = n % 2

        @pl.when(n >= 2)
        def _():
            store(n - 2, slot).wait()

        cols = pl.ds(pl.multiple_of(n * bn, bn), bn)
        for lo in range(0, rows, rows // 2):
            r = slice(lo, lo + rows // 2)
            total = acc_scr[n, r, :] + jnp.dot(recv_scr[r, :], w_scr[i % slots], preferred_element_type=F32)
            o_st[slot, r, :] = (total + x_scr[r, cols].astype(F32)).astype(BF16)
        store(n, slot).start()
        return 0

    lax.fori_loop(0, tiles, other_half, 0)
    for n in range(tiles - 2, tiles):
        store(n, n % 2).wait()
    for i in range(pieces):
        exchange(i).wait_send()


def out_project(keep, send, w_o, x):
    rows, half = keep.shape
    dim = w_o.shape[1]
    bn = 512
    slots = 4
    dma = pltpu.SemaphoreType.DMA
    return pl.pallas_call(
        out_kernel,
        in_specs=[ANY, ANY, ANY, ANY],
        out_specs=ANY,
        scratch_shapes=[
            pltpu.VMEM((rows, half), BF16),
            pltpu.VMEM((rows, half), BF16),
            pltpu.VMEM((rows, dim), BF16),
            pltpu.VMEM((slots, half, bn), BF16),
            pltpu.VMEM((dim // bn, rows, bn), F32),
            pltpu.VMEM((2, rows, bn), BF16),
            dma((8,)), dma, dma((slots,)), dma((4,)), dma((4,)), dma((2,)),
        ],
        out_shape=jax.ShapeDtypeStruct((rows, dim), BF16),
        compiler_params=pltpu.CompilerParams(vmem_limit_bytes=VMEM_LIMIT, collective_id=1, has_side_effects=True),
        cost_estimate=pl.CostEstimate(flops=4 * rows * half * dim, bytes_accessed=4 * half * dim, transcendentals=0),
        name='out_proj',
    )(keep, send, w_o, x)


def solution(mesh):
    def device_step(hidden, ln_gain, w_q, w_k, w_v, w_o, q_gain, k_gain):
        q, k, v = front(hidden, ln_gain, w_q, w_k, w_v, q_gain, k_gain)
        keep, send = attention(q, k, v)
        return out_project(keep, send, w_o, hidden)

    row_spec = P(('dp', 'sp'), None)
    return jax.shard_map(device_step, mesh=mesh, in_specs=(row_spec, P(), P(), P(), P(), P(), P(), P()), out_specs=row_spec, check_vma=False)
```
